256 devices in a mesh: dp: 32 (over y, z), vocab: 8 (over x, core).
Axes of the slice: x: 4, y: 4, z: 8, core: 2. Of those that a mesh axis runs over, the one named last changes fastest.
Arguments:
- hidden_states: bfloat16 [16384, 2048], P('dp', 'vocab'), may hold values from -12 to 12
- teacher_logits: bfloat16 [16384, 16384], P('dp', 'vocab'), may hold values from -24 to 240
- head_weight: bfloat16 [2048, 16384], P(None, 'vocab'), as said below
Outputs:
- kl_per_token: float32 [16384], P('dp')
- hidden_grad: bfloat16 [16384, 2048], P('dp', 'vocab')
- head_grad: float32 [2048, 16384], P('dp', 'vocab')
The draws below stay inside these ranges and needn't reach their ends.
Inputs may be any that keep to these rules, and one draw needn't show every extreme that they name: `head_weight`: every entry's magnitude is at most 18 / sqrt(2048).
All inputs are finite; a program needn't handle non-finite values.
Results may differ from the reference program's by a relative error of at most 0.014.
Values may be sent and summed in bfloat16 or wider, within the bound.
A program may use at most 128 MiB of HBM per device.

```python
import math
import jax
import jax.numpy as jnp
from jax import lax

D = 2048
V = 16384
MICRO = 2
TOK = 256
TOKENS = 16384
N_DP = 32


def head_columns(key):
    column_key = jax.random.fold_in(key, 7101)
    value_key = jax.random.fold_in(column_key, 1)
    spread = 3.0 / math.sqrt(D)
    values = jnp.clip(jax.random.normal(value_key, (D, V), jnp.float32), -6.0, 6.0)
    return values * spread


def draw_head_weight(key, part):
    return head_columns(key).astype(jnp.bfloat16)


def draw_hidden_states(key, part):
    streams = jax.random.split(jax.random.fold_in(key, 7202), 2)
    values = jnp.clip(jax.random.normal(streams[1], (TOKENS, D), jnp.float32), -6.0, 6.0)
    return values.astype(jnp.bfloat16)


def draw_teacher_logits(key, part):
    streams = jax.random.split(jax.random.fold_in(key, 7303), 3)
    values = 3.0 * jnp.clip(jax.random.normal(streams[2], (TOKENS, V), jnp.float32), -8.0, 8.0)
    return values.astype(jnp.bfloat16)


def setup_inputs(seed: int = 0) -> dict:
    key_list = jax.random.split(jax.random.key(seed), 4)
    hidden_states = draw_hidden_states(jax.random.fold_in(key_list[3], 71), 0)
    teacher_logits = draw_teacher_logits(jax.random.fold_in(key_list[3], 71), 0)
    head_weight = draw_head_weight(jax.random.fold_in(key_list[3], 71), 0)
    return {"hidden_states": hidden_states, "teacher_logits": teacher_logits, "head_weight": head_weight}


grad_scale = 8.0


def token_group(hidden_rows, teacher_rows, head_weight):
    student = jnp.dot(hidden_rows, head_weight, preferred_element_type=jnp.float32)
    teacher = teacher_rows.astype(jnp.float32)
    student_max = jnp.max(student, axis=1, keepdims=True)
    teacher_max = jnp.max(teacher, axis=1, keepdims=True)
    student_terms = jnp.exp(student - student_max)
    teacher_terms = jnp.exp(teacher - teacher_max)
    student_total = jnp.sum(student_terms, axis=1)
    teacher_total = jnp.sum(teacher_terms, axis=1)
    cross_term = jnp.sum(teacher_terms * (teacher - student), axis=1)
    divergence = cross_term / teacher_total - teacher_max[:, 0] - jnp.log(teacher_total) + student_max[:, 0] + jnp.log(student_total)
    logit_grad = (grad_scale * (student_terms / student_total[:, None] - teacher_terms / teacher_total[:, None])).astype(jnp.bfloat16)
    hidden_grad = lax.dot_general(logit_grad, head_weight, (((1,), (1,)), ((), ())), preferred_element_type=jnp.float32).astype(jnp.bfloat16)
    group_grad = lax.dot_general(hidden_rows, logit_grad, (((0,), (0,)), ((), ())), preferred_element_type=jnp.float32).astype(jnp.bfloat16)
    return divergence, hidden_grad, group_grad


def reference(hidden_states, teacher_logits, head_weight):
    group_rows = MICRO * TOK
    grouped_hidden = hidden_states.reshape(N_DP, group_rows, D)
    grouped_teacher = teacher_logits.reshape(N_DP, group_rows, V)

    def one_group(running, inputs):
        divergence, hidden_grad, group_grad = token_group(inputs[0], inputs[1], head_weight)
        running = running + lax.optimization_barrier(group_grad).astype(jnp.float32)
        return running, (divergence, hidden_grad)

    head_grad, results = lax.scan(one_group, jnp.zeros((D, V), jnp.float32), (grouped_hidden, grouped_teacher))
    divergence = results[0].reshape(TOKENS)
    hidden_grad = results[1].reshape(TOKENS, D)
    return divergence, hidden_grad, head_grad
```

```python
import jax
import jax.numpy as jnp
from jax import lax
from jax.experimental import pallas as pl
from jax.experimental.pallas import tpu as pltpu
from jax.sharding import Mesh
from jax.sharding import PartitionSpec as P

MESH = pl.DeviceIdType.MESH
F32, BF16 = jnp.float32, jnp.bfloat16
NY, NZ, NX = 4, 8, 4
ROWS, WIDTH, VOCAB, PART = 512, 2048, 2048, 256
GRAD_SCALE = 8.0
LANES = 128

A_WIDTH = 1152
A_SPLIT = (640, 512, 640, 512)
B_SUBS = ((1152, 512, 256), (1664, 384, 128))
A_PAIRS = ((4, 3), (5, 2), (6, 1), (7, 0))


def in_order(ops):
    rate = 46.0e3
    done, arrived, link_free, now, order = {}, {}, {}, 0.0, []
    left = list(ops)
    while left:
        best = None
        for rank, op in enumerate(left):
            if any(d not in done for d in op["after"]) or any(r not in arrived for r in op["recv"]):
                continue
            ready = max([now] + [arrived[r] for r in op["recv"]])
            key = (ready, op["rank"], rank)
            if best is None or key < best[0]:
                best = (key, op)
        (ready, _, _), op = best
        now = ready + op["time"]
        done[op["name"]] = now
        for link, size, key in op["send"]:
            begin = max(now, link_free.get(link, 0.0))
            wire = size / (rate if link != "c" else 600e3)
            link_free[link] = begin + wire
            arrived[key] = begin + wire + (2.0 if link != "c" else 1.0)
        order.append(op)
        left.remove(op)
    return order, now


def fold(op, tiles):
    tiles = list(tiles)
    while len(tiles) > 1:
        pairs = [op(a, b) for a, b in zip(tiles[::2], tiles[1::2])]
        tiles = pairs + ([tiles[-1]] if len(tiles) % 2 else [])
    return tiles[0]


def lane_tiles(value):
    return [value[:, i : i + LANES] for i in range(0, value.shape[1], LANES)]


def pieces(begin, width, step):
    return [(b, min(step, begin + width - b)) for b in range(begin, begin + width, step)]


SCRATCH = dict(
    hid=((8, ROWS, PART), BF16),
    hid_t=((NY, NZ, 64, ROWS), BF16),
    tea=((ROWS, VOCAB), BF16),
    head=((8, PART, VOCAB), BF16),
    stu=((ROWS, VOCAB), F32),
    stu_exp=((ROWS, VOCAB), F32),
    tea_exp=((ROWS, VOCAB), F32),
    grad=((ROWS, VOCAB), BF16),
    part_a=((ROWS, LANES), F32),
    part_b=((ROWS, LANES), F32),
    tea_max=((ROWS, LANES), F32),
    x_tea=((8, 8, LANES), F32),
    x_stu=((8, 8, LANES), F32),
    x_cross=((8, 8, LANES), F32),
    a1_s1=((2, 4, 128, 640), BF16),
    a1_r1=((2, 4, 128, 640), BF16),
    a1_s2=((2, 4, 128, A_WIDTH), BF16),
    a1_r2=((2, 4, 128, A_WIDTH), BF16),
    a1_sum=((8, 64, A_WIDTH), F32),
    a2_s1=((2, 64, 640), BF16),
    a2_r1=((2, 64, 640), BF16),
    a2_s=((2, 3, 64, A_WIDTH), BF16),
    a2_r=((2, 3, 64, A_WIDTH), BF16),
    b1_s1=((2, 2, 256, 256), BF16),
    b1_r1=((2, 2, 256, 256), BF16),
    b1_s=((2, 3, 256, VOCAB - A_WIDTH), BF16),
    b1_r=((2, 3, 256, VOCAB - A_WIDTH), BF16),
    b1_sum=((NY, 64, VOCAB - A_WIDTH), F32),
    b2_s1=((2, 2, 64, 256), BF16),
    b2_r1=((2, 2, 64, 256), BF16),
    b2_s2=((2, 64, VOCAB - A_WIDTH), BF16),
    b2_r2=((2, 64, VOCAB - A_WIDTH), BF16),
    hs_s=((4, ROWS, PART), BF16),
    hs_r=((4, ROWS, PART), BF16),
    h1_s=((2, 256, PART), BF16),
    h1_r=((2, 256, PART), BF16),
    h2_s=((2, ROWS, PART), BF16),
    h2_r=((2, ROWS, PART), BF16),
)
NAMES = tuple(SCRATCH)
N_COPIES = 120


def kernel(hidden_in, teacher_in, head_in, kl_out, hg_out, gh_out, *rest):
    bufs = dict(zip(NAMES, rest))
    load_sem, send_sem, recv_sem = rest[len(NAMES) :]
    hid, hid_t, tea, head, stu = (bufs[k] for k in ("hid", "hid_t", "tea", "head", "stu"))
    stu_exp, tea_exp, grad = bufs["stu_exp"], bufs["tea_exp"], bufs["grad"]
    part_a, part_b, tea_max = bufs["part_a"], bufs["part_b"], bufs["tea_max"]

    y, z, x, c = (lax.axis_index(a) for a in ("y", "z", "x", "c"))

    def near(axis, delta):
        here, size = {"y": (y, NY), "z": (z, NZ), "x": (x, NX)}[axis]
        return lax.rem(here + (delta % size), size)

    def vocab_at(dx, dc):
        return 2 * near("x", dx) + (c if dc == 0 else 1 - c)

    me, sib = vocab_at(0, 0), vocab_at(0, 1)
    to_sib = {"c": 1 - c}
    peers = [(dx, dc) for dx in range(NX) for dc in range(2) if (dx, dc) != (0, 0)]

    def peer(dx, dc):
        return {"x": near("x", dx), "c": c if dc == 0 else 1 - c}

    numbers, sent = {}, []

    def remote(key, src, dst, device):
        number = numbers.setdefault(key, len(numbers))
        assert number < N_COPIES
        return pltpu.make_async_remote_copy(
            src_ref=src,
            dst_ref=dst,
            send_sem=send_sem.at[number],
            recv_sem=recv_sem.at[number],
            device_id=device,
            device_id_type=MESH,
        )

    def send(key, src, dst, device):
        copy = remote(key, src, dst, device)
        copy.start()
        sent.append(copy)

    def arrive(key, dst, device=None):
        remote(key, dst, dst, to_sib).wait_recv()

    loads = [pltpu.make_async_copy(hidden_in, hid.at[me], load_sem.at[0])]
    loads[0].start()
    slots = [vocab_at(*p) for p in ((0, 0), (0, 1), (3, 0), (1, 0), (3, 1), (1, 1), (2, 0), (2, 1))]
    own, sibling, left, right, left_s, right_s, far, far_s = slots
    head_loads = []
    for k, slot in enumerate(slots):
        rows = pl.ds(pl.multiple_of(slot * PART, PART), PART)
        head_loads.append(pltpu.make_async_copy(head_in.at[rows], head.at[slot], load_sem.at[1 + k]))
    tea_load = pltpu.make_async_copy(teacher_in, tea, load_sem.at[9])
    head_loads[0].start()
    head_loads[1].start()
    tea_load.start()
    for copy in head_loads[2:]:
        copy.start()

    barrier = pltpu.get_barrier_semaphore()
    around = [peer(*p) for p in peers] + [{a: near(a, d)} for a in "yz" for d in (1, -1)]
    for device in around:
        pl.semaphore_signal(barrier, inc=1, device_id=device, device_id_type=MESH)
    pl.semaphore_wait(barrier, len(around))

    halves = (pl.ds(0, 256), pl.ds(256, 256))
    x_right, x_left = {"x": near("x", 1)}, {"x": near("x", -1)}
    loads[0].wait()

    def half(slot, h):
        return hid.at[slot, halves[h]]

    def give(key, slot, h, device):
        send(key, half(slot, h), half(slot, h), device)

    give("L0", own, 0, x_right)
    give("R1", own, 1, x_left)
    send("own", hid.at[own], hid.at[own], to_sib)
    give("L1", own, 1, x_right)
    give("R0", own, 0, x_left)

    waited = set()

    def logits(k, begin, rows):
        slot = slots[k]
        if k not in waited:
            head_loads[k].wait()
            waited.add(k)

        @pl.loop(0, VOCAB // 512)
        def _(n):
            cols = pl.ds(pl.multiple_of(n * 512, 512), 512)
            value = jnp.dot(
                hid[slot, begin : begin + rows, :], head[slot, :, cols], preferred_element_type=F32
            )
            if k == 0:
                stu[begin : begin + rows, cols] = value
            else:
                stu[begin : begin + rows, cols] += value

    def row_blocks(size, body):
        @pl.loop(0, ROWS // size)
        def _(n):
            body(pl.ds(pl.multiple_of(n * size, size), size))

    def spread_max(ref_in, ref_out):
        ref_out[...] = jnp.broadcast_to(jnp.max(ref_in[...], axis=1, keepdims=True), (ROWS, LANES))

    def tea_peaks(rows):
        part_a[rows, :] = fold(jnp.maximum, lane_tiles(tea[rows, :].astype(F32)))

    def tea_terms(rows):
        peak = tea_max[rows, :]
        total = None
        for i in range(0, VOCAB, LANES):
            term = jnp.exp(tea[rows, i : i + LANES].astype(F32) - peak)
            tea_exp[rows, i : i + LANES] = term
            total = term if total is None else total + term
        part_b[rows, :] = total

    def compact(ref, slot, at, peaks_ref):
        for b in range(4):
            rows = slice(b * LANES, (b + 1) * LANES)
            if peaks_ref is not None:
                ref[slot, b : b + 1, :] = peaks_ref[rows, :].T[0:1, :]
            ref[slot, at + b : at + b + 1, :] = jnp.sum(part_b[rows, :].T, axis=0, keepdims=True)

    def share(name):
        ref = bufs[name]
        for dx, dc in peers:
            send((name, dx, dc), ref.at[me], ref.at[me], peer(dx, dc))

    def shared(name):
        ref = bufs[name]
        for dx, dc in peers:
            slot = vocab_at(-dx, dc)
            arrive((name, dx, dc), ref.at[slot])

    def merged(ref):
        peak = fold(jnp.maximum, [ref[k, 0:4, :] for k in range(8)])
        total = None
        for k in range(8):
            term = ref[k, 4:8, :] * jnp.exp(ref[k, 0:4, :] - peak)
            total = term if total is None else total + term
        return peak, total

    def spread(value, ref):
        for b in range(4):
            ref[b * LANES : (b + 1) * LANES, :] = jnp.broadcast_to(
                value[b : b + 1, :], (LANES, LANES)
            ).T

    logits(0, 0, ROWS)
    arrive("own", hid.at[sibling])
    logits(1, 0, ROWS)
    tea_load.wait()
    row_blocks(32, tea_peaks)
    spread_max(part_a, tea_max)
    arrive("L0", half(left, 0))
    give("O0", left, 0, x_right)
    give("SL0", left, 0, to_sib)
    arrive("R1", half(right, 1))
    give("O1", right, 1, x_left)
    give("SR1", right, 1, to_sib)
    logits(2, 0, 256)
    logits(3, 256, 256)
    arrive("SL0", half(left_s, 0))
    logits(4, 0, 256)
    arrive("SR1", half(right_s, 1))
    logits(5, 256, 256)
    row_blocks(16, tea_terms)
    arrive("L1", half(left, 1))
    give("SL1", left, 1, to_sib)
    arrive("R0", half(right, 0))
    give("SR0", right, 0, to_sib)
    compact(bufs["x_tea"], me, 4, tea_max)
    share("x_tea")
    logits(2, 256, 256)
    logits(3, 0, 256)
    arrive("SL1", half(left_s, 1))
    logits(4, 256, 256)
    arrive("SR0", half(right_s, 0))
    logits(5, 0, 256)
    arrive("O0", half(far, 0))
    give("SO0", far, 0, to_sib)
    arrive("O1", half(far, 1))
    give("SO1", far, 1, to_sib)
    logits(6, 0, ROWS)
    arrive("SO0", half(far_s, 0))
    arrive("SO1", half(far_s, 1))
    logits(7, 0, ROWS)

    def stu_peaks(rows):
        part_a[rows, :] = fold(jnp.maximum, lane_tiles(stu[rows, :]))

    def stu_terms(rows):
        peak = part_a[rows, :]
        total = None
        for i in range(0, VOCAB, LANES):
            term = jnp.exp(stu[rows, i : i + LANES] - peak)
            stu_exp[rows, i : i + LANES] = term
            total = term if total is None else total + term
        part_b[rows, :] = total

    row_blocks(32, stu_peaks)
    spread_max(part_a, part_a)
    row_blocks(16, stu_terms)
    compact(bufs["x_stu"], me, 4, part_a)
    share("x_stu")

    for k in range(8):
        for b in range(4):
            rows = slice(b * LANES, (b + 1) * LANES)
            turned = hid[k, rows, :].T
            first = (k % 2) * 4
            hid_t[k // 2, first : first + 4, :, rows] = turned.reshape(4, 64, LANES)

    shared("x_tea")
    tea_peak, tea_total = merged(bufs["x_tea"])
    spread(GRAD_SCALE * jnp.exp(bufs["x_tea"][me, 0:4, :] - tea_peak) / tea_total, part_b)
    shared("x_stu")
    stu_peak, stu_total = merged(bufs["x_stu"])
    spread(GRAD_SCALE * jnp.exp(bufs["x_stu"][me, 0:4, :] - stu_peak) / stu_total, part_a)

    def grads(rows):
        stu_scale, tea_scale = part_a[rows, :], part_b[rows, :]
        for i in range(0, VOCAB, LANES):
            cols = slice(i, i + LANES)
            grad[rows, cols] = (stu_exp[rows, cols] * stu_scale - tea_exp[rows, cols] * tea_scale).astype(BF16)

    row_blocks(16, grads)

    ops = []

    def op(name, emit, time, rank, recv=(), send=(), after=()):
        ops.append(
            dict(name=name, emit=emit, time=time, rank=rank, recv=list(recv), send=list(send), after=list(after))
        )

    links = {("y", 0): "y+", ("y", 1): "y-", ("z", 0): "z+", ("z", 1): "z-", ("x", 0): "x+", ("x", 1): "x-"}

    def toward(axis, d):
        return {axis: near(axis, 1 if d == 0 else -1)}

    def signed(d, n):
        return n if d == 0 else -n

    def product(lhs, begin, width):
        return jnp.dot(lhs, grad[:, begin : begin + width], preferred_element_type=F32)

    def half_of(q_split, total, d):
        return (0, q_split) if d == 0 else (q_split, total - q_split)

    def a1_rows(q, dest):
        j = near("y", dest)
        return jnp.concatenate([hid_t[j, near("z", k)] for k in A_PAIRS[q]], axis=0)

    def a1_first(q, d):
        begin, width = half_of(A_SPLIT[q], A_WIDTH, d)
        src, dst = (bufs[n].at[d, q, :, pl.ds(0, width)] for n in ("a1_s1", "a1_r1"))

        def emit():
            lhs = a1_rows(q, 2)
            for b, w in pieces(0, width, 256):
                bufs["a1_s1"][d, q, :, b : b + w] = product(lhs, begin + b, w).astype(BF16)
            send(("a1", q, d, 1), src, dst, toward("y", d))

        op(("a1", q, d, 1), emit, 0.25, 1, send=[(links["y", d], 256 * width, ("a1", q, d, 1))])

    def a1_second(q, d):
        begin, width = half_of(A_SPLIT[q], A_WIDTH, d)

        def emit():
            arrive(("a1", q, d, 1), bufs["a1_r1"].at[d, q, :, pl.ds(0, width)])
            lhs = a1_rows(q, signed(d, 1))
            for b, w in pieces(0, begin, 256) + pieces(begin + width, A_WIDTH - begin - width, 256):
                bufs["a1_s2"][d, q, :, b : b + w] = product(lhs, b, w).astype(BF16)
            for b, w in pieces(begin, width, 256):
                got = bufs["a1_r1"][d, q, :, b - begin : b - begin + w].astype(F32)
                bufs["a1_s2"][d, q, :, b : b + w] = (product(lhs, b, w) + got).astype(BF16)
            send(("a1", q, d, 2), bufs["a1_s2"].at[d, q], bufs["a1_r2"].at[d, q], toward("y", d))

        op(
            ("a1", q, d, 2),
            emit,
            0.45,
            0,
            recv=[("a1", q, d, 1)],
            send=[(links["y", d], 256 * A_WIDTH, ("a1", q, d, 2))],
        )

    def a1_last(q):
        def emit():
            for d in range(2):
                arrive(("a1", q, d, 2), bufs["a1_r2"].at[d, q])
            lhs = a1_rows(q, 0)
            for b, w in pieces(0, A_WIDTH, 256):
                got = [bufs["a1_r2"][d, q, :, b : b + w].astype(F32) for d in range(2)]
                value = product(lhs, b, w) + got[0] + got[1]
                for i, k in enumerate(A_PAIRS[q]):
                    bufs["a1_sum"][k, :, b : b + w] = value[64 * i : 64 * (i + 1), :]

        op(("a1", q), emit, 0.5, 0, recv=[("a1", q, d, 2) for d in range(2)])

    for q in range(4):
        for d in range(2):
            a1_first(q, d)
            a1_second(q, d)
        a1_last(q)

    owner = {k: q for q, pair in enumerate(A_PAIRS) for k in pair}
    a2_split = 640

    def a2_step(d, step):
        begin, width = half_of(a2_split, A_WIDTH, d)
        dest = signed(d, 5 - step) % NZ
        if step == 1:
            src, dst = (bufs[n].at[d, :, pl.ds(0, width)] for n in ("a2_s1", "a2_r1"))
        else:
            src, dst = (bufs[n].at[d, step - 2] for n in ("a2_s", "a2_r"))

        def emit():
            total = bufs["a1_sum"]
            if step == 1:
                bufs["a2_s1"][d, :, 0:width] = total[dest, :, begin : begin + width].astype(BF16)
            elif step == 2:
                arrive(("a2", d, 1), bufs["a2_r1"].at[d, :, pl.ds(0, width)])
                bufs["a2_s"][d, 0] = total[dest].astype(BF16)
                got = bufs["a2_r1"][d, :, 0:width].astype(F32)
                bufs["a2_s"][d, 0, :, begin : begin + width] = (
                    total[dest, :, begin : begin + width] + got
                ).astype(BF16)
            else:
                arrive(("a2", d, step - 1), bufs["a2_r"].at[d, step - 3])
                got = bufs["a2_r"][d, step - 3].astype(F32)
                bufs["a2_s"][d, step - 2] = (total[dest] + got).astype(BF16)
            send(("a2", d, step), src, dst, toward("z", d))

        op(
            ("a2", d, step),
            emit,
            0.15,
            0,
            recv=[("a2", d, step - 1)] if step > 1 else [],
            send=[(links["z", d], 128 * (width if step == 1 else A_WIDTH), ("a2", d, step))],
            after=[("a1", owner[dest])],
        )

    def a2_last():
        def emit():
            for d in range(2):
                arrive(("a2", d, 4), bufs["a2_r"].at[d, 2])
            got = [bufs["a2_r"][d, 2].astype(F32) for d in range(2)]
            gh_out[:, 0:A_WIDTH] = bufs["a1_sum"][0] + got[0] + got[1]

        op("a2", emit, 0.15, 0, recv=[("a2", d, 4) for d in range(2)], after=[("a1", 3)])

    for d in range(2):
        for step in range(1, 5):
            a2_step(d, step)
    a2_last()

    def b1_rows(dest):
        return hid_t[:, near("z", dest)].reshape(256, ROWS)

    def b1_step(i, d, step):
        first, width, cut = B_SUBS[i]
        at = first - A_WIDTH
        begin, half_width = half_of(cut, width, d)
        dest = signed(d, 5 - step)
        cols = pl.ds(at, width)
        if step == 1:
            src, dst = (bufs[n].at[d, i, :, pl.ds(0, half_width)] for n in ("b1_s1", "b1_r1"))
        else:
            src, dst = (bufs[n].at[d, step - 2, :, cols] for n in ("b1_s", "b1_r"))

        def emit():
            lhs = b1_rows(dest)
            if step == 1:
                for b, w in pieces(0, half_width, 256):
                    bufs["b1_s1"][d, i, :, b : b + w] = product(lhs, first + begin + b, w).astype(BF16)
            elif step == 2:
                arrive(("b1", i, d, 1), bufs["b1_r1"].at[d, i, :, pl.ds(0, half_width)])
                for b, w in pieces(0, begin, 256) + pieces(begin + half_width, width - begin - half_width, 256):
                    bufs["b1_s"][d, 0, :, at + b : at + b + w] = product(lhs, first + b, w).astype(BF16)
                for b, w in pieces(begin, half_width, 256):
                    got = bufs["b1_r1"][d, i, :, b - begin : b - begin + w].astype(F32)
                    bufs["b1_s"][d, 0, :, at + b : at + b + w] = (product(lhs, first + b, w) + got).astype(BF16)
            else:
                arrive(("b1", i, d, step - 1), bufs["b1_r"].at[d, step - 3, :, cols])
                for b, w in pieces(0, width, 256):
                    got = bufs["b1_r"][d, step - 3, :, at + b : at + b + w].astype(F32)
                    bufs["b1_s"][d, step - 2, :, at + b : at + b + w] = (
                        product(lhs, first + b, w) + got
                    ).astype(BF16)
            send(("b1", i, d, step), src, dst, toward("z", d))

        op(
            ("b1", i, d, step),
            emit,
            0.3,
            0.5 if step > 1 else 0.9,
            recv=[("b1", i, d, step - 1)] if step > 1 else [],
            send=[(links["z", d], 512 * (half_width if step == 1 else width), ("b1", i, d, step))],
        )

    def b1_last(i):
        first, width, cut = B_SUBS[i]
        at = first - A_WIDTH

        def emit():
            for d in range(2):
                arrive(("b1", i, d, 4), bufs["b1_r"].at[d, 2, :, pl.ds(at, width)])
            lhs = b1_rows(0)
            for b, w in pieces(0, width, 256):
                got = [bufs["b1_r"][d, 2, :, at + b : at + b + w].astype(F32) for d in range(2)]
                value = product(lhs, first + b, w) + got[0] + got[1]
                bufs["b1_sum"][:, :, at + b : at + b + w] = value.reshape(NY, 64, w)

        op(("b1", i), emit, 0.4, 0, recv=[("b1", i, d, 4) for d in range(2)])

    def b2_step(i, d, step):
        first, width, cut = B_SUBS[i]
        at = first - A_WIDTH
        begin, half_width = half_of(cut, width, d)
        dest = signed(d, 3 - step)
        cols = pl.ds(at, width)
        if step == 1:
            src, dst = (bufs[n].at[d, i, :, pl.ds(0, half_width)] for n in ("b2_s1", "b2_r1"))
        else:
            src, dst = (bufs[n].at[d, :, cols] for n in ("b2_s2", "b2_r2"))

        def emit():
            j = near("y", dest)
            total = bufs["b1_sum"]
            mine = slice(at + begin, at + begin + half_width)
            if step == 1:
                bufs["b2_s1"][d, i, :, 0:half_width] = total[j, :, mine].astype(BF16)
            else:
                arrive(("b2", i, d, 1), bufs["b2_r1"].at[d, i, :, pl.ds(0, half_width)])
                bufs["b2_s2"][d, :, at : at + width] = total[j, :, at : at + width].astype(BF16)
                got = bufs["b2_r1"][d, i, :, 0:half_width].astype(F32)
                bufs["b2_s2"][d, :, mine] = (total[j, :, mine] + got).astype(BF16)
            send(("b2", i, d, step), src, dst, toward("y", d))

        op(
            ("b2", i, d, step),
            emit,
            0.1,
            0,
            recv=[("b2", i, d, 1)] if step > 1 else [],
            send=[(links["y", d], 128 * (half_width if step == 1 else width), ("b2", i, d, step))],
            after=[("b1", i)],
        )

    def b2_last(i):
        first, width, cut = B_SUBS[i]
        cols = slice(first - A_WIDTH, first - A_WIDTH + width)

        def emit():
            for d in range(2):
                arrive(("b2", i, d, 2), bufs["b2_r2"].at[d, :, pl.ds(first - A_WIDTH, width)])
            got = [bufs["b2_r2"][d, :, cols].astype(F32) for d in range(2)]
            gh_out[:, first : first + width] = bufs["b1_sum"][y, :, cols] + got[0] + got[1]

        op(("b2", i), emit, 0.1, 0, recv=[("b2", i, d, 2) for d in range(2)], after=[("b1", i)])

    for i in range(len(B_SUBS)):
        for d in range(2):
            for step in range(1, 5):
                b1_step(i, d, step)
        b1_last(i)
        for d in range(2):
            for step in (1, 2):
                b2_step(i, d, step)
        b2_last(i)

    hops = (2, 1, 3, 0)

    def back(slot, h):
        return lax.dot_general(
            grad[halves[h], :], head[slot], (((1,), (1,)), ((), ())), preferred_element_type=F32
        )

    def hs_step(n):
        def emit():
            slot = vocab_at(hops[n], 1)
            for h in range(2):
                bufs["hs_s"][n, halves[h], :] = back(slot, h).astype(BF16)
            send(("hs", n), bufs["hs_s"].at[n], bufs["hs_r"].at[n], to_sib)

        op(("hs", n), emit, 0.9, 3, send=[("c", 262144, ("hs", n))])

    def hg_step(n):
        def emit():
            arrive(("hs", n), bufs["hs_r"].at[n])
            if n == 1 or n == 2:
                d = n - 1
                arrive(("h1", d), bufs["h1_r"].at[d])
            if n == 3:
                for d in range(2):
                    arrive(("h2", d), bufs["h2_r"].at[d])
            slot = vocab_at(hops[n], 0)
            for h in range(2):
                rows = halves[h]
                value = back(slot, h) + bufs["hs_r"][n, rows, :].astype(F32)
                if n == 0:
                    bufs["h1_s"][h] = value.astype(BF16)
                    send(("h1", h), bufs["h1_s"].at[h], bufs["h1_r"].at[h], toward("x", h))
                elif n < 3:
                    if h == n - 1:
                        value = value + bufs["h1_r"][h].astype(F32)
                    bufs["h2_s"][n - 1, rows, :] = value.astype(BF16)
                else:
                    got = [bufs["h2_r"][d, rows, :].astype(F32) for d in range(2)]
                    hg_out[rows, :] = (value + got[0] + got[1]).astype(BF16)
            if n == 1 or n == 2:
                d = n - 1
                send(("h2", d), bufs["h2_s"].at[d], bufs["h2_r"].at[d], toward("x", d))

        recv = [("hs", n)] + {0: [], 1: [("h1", 0)], 2: [("h1", 1)], 3: [("h2", 0), ("h2", 1)]}[n]
        sends = {
            0: [("x+", 131072, ("h1", 0)), ("x-", 131072, ("h1", 1))],
            1: [("x+", 262144, ("h2", 0))],
            2: [("x-", 262144, ("h2", 1))],
            3: [],
        }[n]
        op(("hg", n), emit, 1.0, 3, recv=recv, send=sends)

    for n in range(4):
        hs_step(n)
        hg_step(n)

    def cross_share():
        def emit():
            def terms(rows):
                total = None
                for i in range(0, VOCAB, LANES):
                    cols = slice(i, i + LANES)
                    term = tea_exp[rows, cols] * (tea[rows, cols].astype(F32) - stu[rows, cols])
                    total = term if total is None else total + term
                part_b[rows, :] = total

            row_blocks(16, terms)
            ref = bufs["x_cross"]
            ref[me, 4:8, :] = jnp.zeros((4, LANES), F32)
            compact(ref, me, 0, None)
            share("x_cross")

        op("cross", emit, 1.5, 4)

    def divergence():
        def emit():
            shared("x_cross")
            ref, peaks = bufs["x_cross"], bufs["x_tea"]
            peak, total = merged(peaks)
            s_peak, s_total = merged(bufs["x_stu"])
            cross = None
            for k in range(8):
                term = ref[k, 0:4, :] * jnp.exp(peaks[k, 0:4, :] - peak)
                cross = term if cross is None else cross + term
            kl_out[...] = cross / total - peak - jnp.log(total) + s_peak + jnp.log(s_total)

        op("kl", emit, 0.3, 5, after=["cross", ("hg", 3)])

    cross_share()
    divergence()

    order, _ = in_order(ops)
    for step in order:
        step["emit"]()

    for copy in sent:
        copy.wait_send()


def per_device(hidden_states, teacher_logits, head_weight):
    vmem = pl.BlockSpec(memory_space=pltpu.VMEM)
    hbm = pl.BlockSpec(memory_space=pl.ANY)
    kl, hidden_grad, head_grad = pl.pallas_call(
        kernel,
        out_shape=(
            jax.ShapeDtypeStruct((4, LANES), F32),
            jax.ShapeDtypeStruct((ROWS, PART), BF16),
            jax.ShapeDtypeStruct((64, VOCAB), F32),
        ),
        in_specs=[hbm, hbm, hbm],
        out_specs=(vmem, vmem, vmem),
        scratch_shapes=[pltpu.VMEM(*SCRATCH[k]) for k in NAMES]
        + [
            pltpu.SemaphoreType.DMA((10,)),
            pltpu.SemaphoreType.DMA((N_COPIES,)),
            pltpu.SemaphoreType.DMA((N_COPIES,)),
        ],
        compiler_params=pltpu.CompilerParams(
            collective_id=0, has_side_effects=True, vmem_limit_bytes=66_000_000
        ),
    )(hidden_states, teacher_logits, head_weight)
    return kl.reshape(ROWS), hidden_grad, head_grad


def solution(mesh):
    split = Mesh(mesh.devices.reshape(NY, NZ, NX, 2), ("y", "z", "x", "c"))
    dp, vocab = ("y", "z"), ("x", "c")
    return jax.shard_map(
        per_device,
        mesh=split,
        in_specs=(P(dp, vocab), P(dp, vocab), P(None, vocab)),
        out_specs=(P(dp), P(dp, vocab), P(dp, vocab)),
        check_vma=False,
    )
```

```python
import jax
import jax.numpy as jnp
from jax import lax
from jax.experimental import pallas as pl
from jax.experimental.pallas import tpu as pltpu
from jax.sharding import Mesh
from jax.sharding import PartitionSpec as P

MESH = pl.DeviceIdType.MESH
F32, BF16 = jnp.float32, jnp.bfloat16
NY, NZ, NX = 4, 8, 4
ROWS, WIDTH, VOCAB, PART = 512, 2048, 2048, 256
GRAD_SCALE = 8.0
LANES = 128

A_WIDTH = 1152
A_SPLIT = (640, 512, 640, 512)
B_SUBS = ((1152, 512, 256), (1664, 384, 128))
A_PAIRS = ((4, 3), (5, 2), (6, 1), (7, 0))


def in_order(ops):
    rate = 46.0e3
    done, arrived, link_free, now, order = {}, {}, {}, 0.0, []
    left = list(ops)
    while left:
        best = None
        for rank, op in enumerate(left):
            if any(d not in done for d in op["after"]) or any(r not in arrived for r in op["recv"]):
                continue
            ready = max([now] + [arrived[r] for r in op["recv"]])
            key = (ready, op["rank"], rank)
            if best is None or key < best[0]:
                best = (key, op)
        (ready, _, _), op = best
        now = ready + op["time"]
        done[op["name"]] = now
        for link, size, key in op["send"]:
            begin = max(now, link_free.get(link, 0.0))
            wire = size / (rate if link != "c" else 600e3)
            link_free[link] = begin + wire
            arrived[key] = begin + wire + (2.0 if link != "c" else 1.0)
        order.append(op)
        left.remove(op)
    return order, now


def fold(op, tiles):
    tiles = list(tiles)
    while len(tiles) > 1:
        pairs = [op(a, b) for a, b in zip(tiles[::2], tiles[1::2])]
        tiles = pairs + ([tiles[-1]] if len(tiles) % 2 else [])
    return tiles[0]


def lane_tiles(value):
    return [value[:, i : i + LANES] for i in range(0, value.shape[1], LANES)]


def pieces(begin, width, step):
    return [(b, min(step, begin + width - b)) for b in range(begin, begin + width, step)]


SCRATCH = dict(
    hid=((8, ROWS, PART), BF16),
    hid_t=((NY, NZ, 64, ROWS), BF16),
    tea=((ROWS, VOCAB), BF16),
    head=((8, PART, VOCAB), BF16),
    stu=((ROWS, VOCAB), F32),
    stu_exp=((ROWS, VOCAB), F32),
    tea_exp=((ROWS, VOCAB), F32),
    grad=((ROWS, VOCAB), BF16),
    part_a=((ROWS, LANES), F32),
    part_b=((ROWS, LANES), F32),
    tea_max=((ROWS, LANES), F32),
    x_tea=((8, 8, LANES), F32),
    x_stu=((8, 8, LANES), F32),
    x_cross=((8, 8, LANES), F32),
    a1_s1=((2, 4, 128, 640), BF16),
    a1_r1=((2, 4, 128, 640), BF16),
    a1_s2=((2, 4, 128, A_WIDTH), BF16),
    a1_r2=((2, 4, 128, A_WIDTH), BF16),
    a1_sum=((8, 64, A_WIDTH), F32),
    a2_s1=((2, 64, 640), BF16),
    a2_r1=((2, 64, 640), BF16),
    a2_s=((2, 3, 64, A_WIDTH), BF16),
    a2_r=((2, 3, 64, A_WIDTH), BF16),
    b1_s1=((2, 2, 256, 256), BF16),
    b1_r1=((2, 2, 256, 256), BF16),
    b1_s=((2, 3, 256, VOCAB - A_WIDTH), BF16),
    b1_r=((2, 3, 256, VOCAB - A_WIDTH), BF16),
    b1_sum=((NY, 64, VOCAB - A_WIDTH), F32),
    b2_s1=((2, 2, 64, 256), BF16),
    b2_r1=((2, 2, 64, 256), BF16),
    b2_s2=((2, 64, VOCAB - A_WIDTH), BF16),
    b2_r2=((2, 64, VOCAB - A_WIDTH), BF16),
    hs_s=((4, ROWS, PART), BF16),
    hs_r=((4, ROWS, PART), BF16),
    h1_s=((2, 256, PART), BF16),
    h1_r=((2, 256, PART), BF16),
    h2_s=((2, ROWS, PART), BF16),
    h2_r=((2, ROWS, PART), BF16),
)
NAMES = tuple(SCRATCH)
N_COPIES = 120
LOAD_ORDER = (0, 3, 1, 2)


def kernel(hidden_in, teacher_in, head_in, kl_out, hg_out, gh_out, *rest):
    bufs = dict(zip(NAMES, rest))
    load_sem, send_sem, recv_sem = rest[len(NAMES) :]
    hid, hid_t, tea, head, stu = (bufs[k] for k in ("hid", "hid_t", "tea", "head", "stu"))
    stu_exp, tea_exp, grad = bufs["stu_exp"], bufs["tea_exp"], bufs["grad"]
    part_a, part_b, tea_max = bufs["part_a"], bufs["part_b"], bufs["tea_max"]

    y, z, x, c = (lax.axis_index(a) for a in ("y", "z", "x", "c"))

    def near(axis, delta):
        here, size = {"y": (y, NY), "z": (z, NZ), "x": (x, NX)}[axis]
        return lax.rem(here + (delta % size), size)

    def vocab_at(dx, dc):
        return 2 * near("x", dx) + (c if dc == 0 else 1 - c)

    me, sib = vocab_at(0, 0), vocab_at(0, 1)
    to_sib = {"c": 1 - c}
    peers = [(dx, dc) for dx in range(NX) for dc in range(2) if (dx, dc) != (0, 0)]

    def peer(dx, dc):
        return {"x": near("x", dx), "c": c if dc == 0 else 1 - c}

    numbers, sent = {}, []

    def remote(key, src, dst, device):
        number = numbers.setdefault(key, len(numbers))
        assert number < N_COPIES
        return pltpu.make_async_remote_copy(
            src_ref=src,
            dst_ref=dst,
            send_sem=send_sem.at[number],
            recv_sem=recv_sem.at[number],
            device_id=device,
            device_id_type=MESH,
        )

    def send(key, src, dst, device):
        copy = remote(key, src, dst, device)
        copy.start()
        sent.append(copy)

    def arrive(key, dst, device=None):
        remote(key, dst, dst, to_sib).wait_recv()

    loads = [pltpu.make_async_copy(hidden_in, hid.at[me], load_sem.at[0])]
    loads[0].start()
    slots = [vocab_at(*p) for k in LOAD_ORDER for p in ((k, 0), (k, 1))]
    own, sibling, left, left_s, right, right_s, far, far_s = slots
    head_loads = []
    for k, slot in enumerate(slots):
        rows = pl.ds(pl.multiple_of(slot * PART, PART), PART)
        head_loads.append(pltpu.make_async_copy(head_in.at[rows], head.at[slot], load_sem.at[1 + k]))
    tea_load = pltpu.make_async_copy(teacher_in, tea, load_sem.at[9])
    head_loads[0].start()
    head_loads[1].start()
    tea_load.start()
    for copy in head_loads[2:]:
        copy.start()

    barrier = pltpu.get_barrier_semaphore()
    around = [peer(*p) for p in peers] + [{a: near(a, d)} for a in "yz" for d in (1, -1)]
    for device in around:
        pl.semaphore_signal(barrier, inc=1, device_id=device, device_id_type=MESH)
    pl.semaphore_wait(barrier, len(around))

    halves = (pl.ds(0, 256), pl.ds(256, 256))
    x_right, x_left = {"x": near("x", 1)}, {"x": near("x", -1)}
    loads[0].wait()

    def half(slot, h):
        return hid.at[slot, halves[h]]

    def give(key, slot, h, device):
        send(key, half(slot, h), half(slot, h), device)

    give("L0", own, 0, x_right)
    give("R1", own, 1, x_left)
    send("own", hid.at[own], hid.at[own], to_sib)
    give("L1", own, 1, x_right)
    give("R0", own, 0, x_left)

    def logits(k, first=False):
        chip = near("x", k)
        for n in range(2):
            head_loads[2 * LOAD_ORDER.index(k) + n].wait()

        @pl.loop(0, VOCAB // 512)
        def _(n):
            cols = pl.ds(pl.multiple_of(n * 512, 512), 512)
            lhs = jnp.concatenate([hid[2 * chip], hid[2 * chip + 1]], axis=1)
            rhs = head[pl.ds(2 * chip, 2), :, cols].reshape(2 * PART, 512)
            value = jnp.dot(lhs, rhs, preferred_element_type=F32)
            if first:
                stu[:, cols] = value
            else:
                stu[:, cols] += value

    def row_blocks(size, body):
        @pl.loop(0, ROWS // size)
        def _(n):
            body(pl.ds(pl.multiple_of(n * size, size), size))

    def spread_max(ref_in, ref_out):
        ref_out[...] = jnp.broadcast_to(jnp.max(ref_in[...], axis=1, keepdims=True), (ROWS, LANES))

    def tea_peaks(rows):
        part_a[rows, :] = fold(jnp.maximum, lane_tiles(tea[rows, :].astype(F32)))

    def tea_terms(rows):
        peak = tea_max[rows, :]
        total = None
        for i in range(0, VOCAB, LANES):
            term = jnp.exp(tea[rows, i : i + LANES].astype(F32) - peak)
            tea_exp[rows, i : i + LANES] = term
            total = term if total is None else total + term
        part_b[rows, :] = total

    def compact(ref, slot, at, peaks_ref):
        for b in range(4):
            rows = slice(b * LANES, (b + 1) * LANES)
            if peaks_ref is not None:
                ref[slot, b : b + 1, :] = peaks_ref[rows, :].T[0:1, :]
            ref[slot, at + b : at + b + 1, :] = jnp.sum(part_b[rows, :].T, axis=0, keepdims=True)

    def share(name):
        ref = bufs[name]
        for dx, dc in peers:
            send((name, dx, dc), ref.at[me], ref.at[me], peer(dx, dc))

    def shared(name):
        ref = bufs[name]
        for dx, dc in peers:
            slot = vocab_at(-dx, dc)
            arrive((name, dx, dc), ref.at[slot])

    def merged(ref):
        peak = fold(jnp.maximum, [ref[k, 0:4, :] for k in range(8)])
        total = None
        for k in range(8):
            term = ref[k, 4:8, :] * jnp.exp(ref[k, 0:4, :] - peak)
            total = term if total is None else total + term
        return peak, total

    def spread(value, ref):
        for b in range(4):
            ref[b * LANES : (b + 1) * LANES, :] = jnp.broadcast_to(
                value[b : b + 1, :], (LANES, LANES)
            ).T

    arrive("own", hid.at[sibling])
    logits(0, first=True)
    tea_load.wait()
    row_blocks(32, tea_peaks)
    spread_max(part_a, tea_max)
    arrive("L0", half(left, 0))
    give("O0", left, 0, x_right)
    give("SL0", left, 0, to_sib)
    arrive("R1", half(right, 1))
    give("O1", right, 1, x_left)
    give("SR1", right, 1, to_sib)
    row_blocks(16, tea_terms)
    arrive("L1", half(left, 1))
    give("SL1", left, 1, to_sib)
    arrive("R0", half(right, 0))
    give("SR0", right, 0, to_sib)
    compact(bufs["x_tea"], me, 4, tea_max)
    share("x_tea")
    arrive("SL0", half(left_s, 0))
    arrive("SL1", half(left_s, 1))
    logits(3)
    arrive("O0", half(far, 0))
    give("SO0", far, 0, to_sib)
    arrive("O1", half(far, 1))
    give("SO1", far, 1, to_sib)
    arrive("SR0", half(right_s, 0))
    arrive("SR1", half(right_s, 1))
    logits(1)
    arrive("SO0", half(far_s, 0))
    arrive("SO1", half(far_s, 1))
    logits(2)

    def stu_peaks(rows):
        part_a[rows, :] = fold(jnp.maximum, lane_tiles(stu[rows, :]))

    def stu_terms(rows):
        peak = part_a[rows, :]
        total = None
        for i in range(0, VOCAB, LANES):
            term = jnp.exp(stu[rows, i : i + LANES] - peak)
            stu_exp[rows, i : i + LANES] = term
            total = term if total is None else total + term
        part_b[rows, :] = total

    row_blocks(32, stu_peaks)
    spread_max(part_a, part_a)
    row_blocks(16, stu_terms)
    compact(bufs["x_stu"], me, 4, part_a)
    share("x_stu")

    for k in range(8):
        for b in range(4):
            rows = slice(b * LANES, (b + 1) * LANES)
            turned = hid[k, rows, :].T
            first = (k % 2) * 4
            hid_t[k // 2, first : first + 4, :, rows] = turned.reshape(4, 64, LANES)

    shared("x_tea")
    tea_peak, tea_total = merged(bufs["x_tea"])
    spread(GRAD_SCALE * jnp.exp(bufs["x_tea"][me, 0:4, :] - tea_peak) / tea_total, part_b)
    shared("x_stu")
    stu_peak, stu_total = merged(bufs["x_stu"])
    spread(GRAD_SCALE * jnp.exp(bufs["x_stu"][me, 0:4, :] - stu_peak) / stu_total, part_a)

    def grads(rows):
        stu_scale, tea_scale = part_a[rows, :], part_b[rows, :]
        for i in range(0, VOCAB, LANES):
            cols = slice(i, i + LANES)
            grad[rows, cols] = (stu_exp[rows, cols] * stu_scale - tea_exp[rows, cols] * tea_scale).astype(BF16)

    row_blocks(16, grads)

    ops = []

    def op(name, emit, time, rank, recv=(), send=(), after=()):
        ops.append(
            dict(name=name, emit=emit, time=time, rank=rank, recv=list(recv), send=list(send), after=list(after))
        )

    links = {("y", 0): "y+", ("y", 1): "y-", ("z", 0): "z+", ("z", 1): "z-", ("x", 0): "x+", ("x", 1): "x-"}

    def toward(axis, d):
        return {axis: near(axis, 1 if d == 0 else -1)}

    def signed(d, n):
        return n if d == 0 else -n

    def product(lhs, begin, width):
        return jnp.dot(lhs, grad[:, begin : begin + width], preferred_element_type=F32)

    def half_of(q_split, total, d):
        return (0, q_split) if d == 0 else (q_split, total - q_split)

    def a1_rows(q, dest):
        j = near("y", dest)
        return jnp.concatenate([hid_t[j, near("z", k)] for k in A_PAIRS[q]], axis=0)

    def a1_first(q, d):
        begin, width = half_of(A_SPLIT[q], A_WIDTH, d)
        src, dst = (bufs[n].at[d, q, :, pl.ds(0, width)] for n in ("a1_s1", "a1_r1"))

        def emit():
            lhs = a1_rows(q, 2)
            for b, w in pieces(0, width, 256):
                bufs["a1_s1"][d, q, :, b : b + w] = product(lhs, begin + b, w).astype(BF16)
            send(("a1", q, d, 1), src, dst, toward("y", d))

        op(("a1", q, d, 1), emit, 0.25, 1, send=[(links["y", d], 256 * width, ("a1", q, d, 1))])

    def a1_second(q, d):
        begin, width = half_of(A_SPLIT[q], A_WIDTH, d)

        def emit():
            arrive(("a1", q, d, 1), bufs["a1_r1"].at[d, q, :, pl.ds(0, width)])
            lhs = a1_rows(q, signed(d, 1))
            for b, w in pieces(0, begin, 256) + pieces(begin + width, A_WIDTH - begin - width, 256):
                bufs["a1_s2"][d, q, :, b : b + w] = product(lhs, b, w).astype(BF16)
            for b, w in pieces(begin, width, 256):
                got = bufs["a1_r1"][d, q, :, b - begin : b - begin + w].astype(F32)
                bufs["a1_s2"][d, q, :, b : b + w] = (product(lhs, b, w) + got).astype(BF16)
            send(("a1", q, d, 2), bufs["a1_s2"].at[d, q], bufs["a1_r2"].at[d, q], toward("y", d))

        op(
            ("a1", q, d, 2),
            emit,
            0.45,
            0,
            recv=[("a1", q, d, 1)],
            send=[(links["y", d], 256 * A_WIDTH, ("a1", q, d, 2))],
        )

    def a1_last(q):
        def emit():
            for d in range(2):
                arrive(("a1", q, d, 2), bufs["a1_r2"].at[d, q])
            lhs = a1_rows(q, 0)
            for b, w in pieces(0, A_WIDTH, 256):
                got = [bufs["a1_r2"][d, q, :, b : b + w].astype(F32) for d in range(2)]
                value = product(lhs, b, w) + got[0] + got[1]
                for i, k in enumerate(A_PAIRS[q]):
                    bufs["a1_sum"][k, :, b : b + w] = value[64 * i : 64 * (i + 1), :]

        op(("a1", q), emit, 0.5, 0, recv=[("a1", q, d, 2) for d in range(2)])

    for q in range(4):
        for d in range(2):
            a1_first(q, d)
            a1_second(q, d)
        a1_last(q)

    owner = {k: q for q, pair in enumerate(A_PAIRS) for k in pair}
    a2_split = 640

    def a2_step(d, step):
        begin, width = half_of(a2_split, A_WIDTH, d)
        dest = signed(d, 5 - step) % NZ
        if step == 1:
            src, dst = (bufs[n].at[d, :, pl.ds(0, width)] for n in ("a2_s1", "a2_r1"))
        else:
            src, dst = (bufs[n].at[d, step - 2] for n in ("a2_s", "a2_r"))

        def emit():
            total = bufs["a1_sum"]
            if step == 1:
                bufs["a2_s1"][d, :, 0:width] = total[dest, :, begin : begin + width].astype(BF16)
            elif step == 2:
                arrive(("a2", d, 1), bufs["a2_r1"].at[d, :, pl.ds(0, width)])
                bufs["a2_s"][d, 0] = total[dest].astype(BF16)
                got = bufs["a2_r1"][d, :, 0:width].astype(F32)
                bufs["a2_s"][d, 0, :, begin : begin + width] = (
                    total[dest, :, begin : begin + width] + got
                ).astype(BF16)
            else:
                arrive(("a2", d, step - 1), bufs["a2_r"].at[d, step - 3])
                got = bufs["a2_r"][d, step - 3].astype(F32)
                bufs["a2_s"][d, step - 2] = (total[dest] + got).astype(BF16)
            send(("a2", d, step), src, dst, toward("z", d))

        op(
            ("a2", d, step),
            emit,
            0.15,
            0,
            recv=[("a2", d, step - 1)] if step > 1 else [],
            send=[(links["z", d], 128 * (width if step == 1 else A_WIDTH), ("a2", d, step))],
            after=[("a1", owner[dest])],
        )

    def a2_last():
        def emit():
            for d in range(2):
                arrive(("a2", d, 4), bufs["a2_r"].at[d, 2])
            got = [bufs["a2_r"][d, 2].astype(F32) for d in range(2)]
            gh_out[:, 0:A_WIDTH] = bufs["a1_sum"][0] + got[0] + got[1]

        op("a2", emit, 0.15, 0, recv=[("a2", d, 4) for d in range(2)], after=[("a1", 3)])

    for d in range(2):
        for step in range(1, 5):
            a2_step(d, step)
    a2_last()

    def b1_rows(dest):
        return hid_t[:, near("z", dest)].reshape(256, ROWS)

    def b1_step(i, d, step):
        first, width, cut = B_SUBS[i]
        at = first - A_WIDTH
        begin, half_width = half_of(cut, width, d)
        dest = signed(d, 5 - step)
        cols = pl.ds(at, width)
        if step == 1:
            src, dst = (bufs[n].at[d, i, :, pl.ds(0, half_width)] for n in ("b1_s1", "b1_r1"))
        else:
            src, dst = (bufs[n].at[d, step - 2, :, cols] for n in ("b1_s", "b1_r"))

        def emit():
            lhs = b1_rows(dest)
            if step == 1:
                for b, w in pieces(0, half_width, 256):
                    bufs["b1_s1"][d, i, :, b : b + w] = product(lhs, first + begin + b, w).astype(BF16)
            elif step == 2:
                arrive(("b1", i, d, 1), bufs["b1_r1"].at[d, i, :, pl.ds(0, half_width)])
                for b, w in pieces(0, begin, 256) + pieces(begin + half_width, width - begin - half_width, 256):
                    bufs["b1_s"][d, 0, :, at + b : at + b + w] = product(lhs, first + b, w).astype(BF16)
                for b, w in pieces(begin, half_width, 256):
                    got = bufs["b1_r1"][d, i, :, b - begin : b - begin + w].astype(F32)
                    bufs["b1_s"][d, 0, :, at + b : at + b + w] = (product(lhs, first + b, w) + got).astype(BF16)
            else:
                arrive(("b1", i, d, step - 1), bufs["b1_r"].at[d, step - 3, :, cols])
                for b, w in pieces(0, width, 256):
                    got = bufs["b1_r"][d, step - 3, :, at + b : at + b + w].astype(F32)
                    bufs["b1_s"][d, step - 2, :, at + b : at + b + w] = (
                        product(lhs, first + b, w) + got
                    ).astype(BF16)
            send(("b1", i, d, step), src, dst, toward("z", d))

        op(
            ("b1", i, d, step),
            emit,
            0.3,
            0.5 if step > 1 else 0.9,
            recv=[("b1", i, d, step - 1)] if step > 1 else [],
            send=[(links["z", d], 512 * (half_width if step == 1 else width), ("b1", i, d, step))],
        )

    def b1_last(i):
        first, width, cut = B_SUBS[i]
        at = first - A_WIDTH

        def emit():
            for d in range(2):
                arrive(("b1", i, d, 4), bufs["b1_r"].at[d, 2, :, pl.ds(at, width)])
            lhs = b1_rows(0)
            for b, w in pieces(0, width, 256):
                got = [bufs["b1_r"][d, 2, :, at + b : at + b + w].astype(F32) for d in range(2)]
                value = product(lhs, first + b, w) + got[0] + got[1]
                bufs["b1_sum"][:, :, at + b : at + b + w] = value.reshape(NY, 64, w)

        op(("b1", i), emit, 0.4, 0, recv=[("b1", i, d, 4) for d in range(2)])

    def b2_step(i, d, step):
        first, width, cut = B_SUBS[i]
        at = first - A_WIDTH
        begin, half_width = half_of(cut, width, d)
        dest = signed(d, 3 - step)
        cols = pl.ds(at, width)
        if step == 1:
            src, dst = (bufs[n].at[d, i, :, pl.ds(0, half_width)] for n in ("b2_s1", "b2_r1"))
        else:
            src, dst = (bufs[n].at[d, :, cols] for n in ("b2_s2", "b2_r2"))

        def emit():
            j = near("y", dest)
            total = bufs["b1_sum"]
            mine = slice(at + begin, at + begin + half_width)
            if step == 1:
                bufs["b2_s1"][d, i, :, 0:half_width] = total[j, :, mine].astype(BF16)
            else:
                arrive(("b2", i, d, 1), bufs["b2_r1"].at[d, i, :, pl.ds(0, half_width)])
                bufs["b2_s2"][d, :, at : at + width] = total[j, :, at : at + width].astype(BF16)
                got = bufs["b2_r1"][d, i, :, 0:half_width].astype(F32)
                bufs["b2_s2"][d, :, mine] = (total[j, :, mine] + got).astype(BF16)
            send(("b2", i, d, step), src, dst, toward("y", d))

        op(
            ("b2", i, d, step),
            emit,
            0.1,
            0,
            recv=[("b2", i, d, 1)] if step > 1 else [],
            send=[(links["y", d], 128 * (half_width if step == 1 else width), ("b2", i, d, step))],
            after=[("b1", i)],
        )

    def b2_last(i):
        first, width, cut = B_SUBS[i]
        cols = slice(first - A_WIDTH, first - A_WIDTH + width)

        def emit():
            for d in range(2):
                arrive(("b2", i, d, 2), bufs["b2_r2"].at[d, :, pl.ds(first - A_WIDTH, width)])
            got = [bufs["b2_r2"][d, :, cols].astype(F32) for d in range(2)]
            gh_out[:, first : first + width] = bufs["b1_sum"][y, :, cols] + got[0] + got[1]

        op(("b2", i), emit, 0.1, 0, recv=[("b2", i, d, 2) for d in range(2)], after=[("b1", i)])

    for i in range(len(B_SUBS)):
        for d in range(2):
            for step in range(1, 5):
                b1_step(i, d, step)
        b1_last(i)
        for d in range(2):
            for step in (1, 2):
                b2_step(i, d, step)
        b2_last(i)

    hops = (2, 1, 3, 0)

    def back(slot, h):
        return lax.dot_general(
            grad[halves[h], :], head[slot], (((1,), (1,)), ((), ())), preferred_element_type=F32
        )

    def hs_step(n):
        def emit():
            slot = vocab_at(hops[n], 1)
            for h in range(2):
                bufs["hs_s"][n, halves[h], :] = back(slot, h).astype(BF16)
            send(("hs", n), bufs["hs_s"].at[n], bufs["hs_r"].at[n], to_sib)

        op(("hs", n), emit, 0.9, 3, send=[("c", 262144, ("hs", n))])

    def hg_step(n):
        def emit():
            arrive(("hs", n), bufs["hs_r"].at[n])
            if n == 1 or n == 2:
                d = n - 1
                arrive(("h1", d), bufs["h1_r"].at[d])
            if n == 3:
                for d in range(2):
                    arrive(("h2", d), bufs["h2_r"].at[d])
            slot = vocab_at(hops[n], 0)
            for h in range(2):
                rows = halves[h]
                value = back(slot, h) + bufs["hs_r"][n, rows, :].astype(F32)
                if n == 0:
                    bufs["h1_s"][h] = value.astype(BF16)
                    send(("h1", h), bufs["h1_s"].at[h], bufs["h1_r"].at[h], toward("x", h))
                elif n < 3:
                    if h == n - 1:
                        value = value + bufs["h1_r"][h].astype(F32)
                    bufs["h2_s"][n - 1, rows, :] = value.astype(BF16)
                else:
                    got = [bufs["h2_r"][d, rows, :].astype(F32) for d in range(2)]
                    hg_out[rows, :] = (value + got[0] + got[1]).astype(BF16)
            if n == 1 or n == 2:
                d = n - 1
                send(("h2", d), bufs["h2_s"].at[d], bufs["h2_r"].at[d], toward("x", d))

        recv = [("hs", n)] + {0: [], 1: [("h1", 0)], 2: [("h1", 1)], 3: [("h2", 0), ("h2", 1)]}[n]
        sends = {
            0: [("x+", 131072, ("h1", 0)), ("x-", 131072, ("h1", 1))],
            1: [("x+", 262144, ("h2", 0))],
            2: [("x-", 262144, ("h2", 1))],
            3: [],
        }[n]
        op(("hg", n), emit, 1.0, 3, recv=recv, send=sends)

    for n in range(4):
        hs_step(n)
        hg_step(n)

    def cross_share():
        def emit():
            def terms(rows):
                total = None
                for i in range(0, VOCAB, LANES):
                    cols = slice(i, i + LANES)
                    term = tea_exp[rows, cols] * (tea[rows, cols].astype(F32) - stu[rows, cols])
                    total = term if total is None else total + term
                part_b[rows, :] = total

            row_blocks(16, terms)
            ref = bufs["x_cross"]
            ref[me, 4:8, :] = jnp.zeros((4, LANES), F32)
            compact(ref, me, 0, None)
            share("x_cross")

        op("cross", emit, 1.5, 4)

    def divergence():
        def emit():
            shared("x_cross")
            ref, peaks = bufs["x_cross"], bufs["x_tea"]
            peak, total = merged(peaks)
            s_peak, s_total = merged(bufs["x_stu"])
            cross = None
            for k in range(8):
                term = ref[k, 0:4, :] * jnp.exp(peaks[k, 0:4, :] - peak)
                cross = term if cross is None else cross + term
            kl_out[...] = cross / total - peak - jnp.log(total) + s_peak + jnp.log(s_total)

        op("kl", emit, 0.3, 5, after=["cross", ("hg", 3)])

    cross_share()
    divergence()

    order, _ = in_order(ops)
    for step in order:
        step["emit"]()

    for copy in sent:
        copy.wait_send()


def handed_on(*refs):
    for src, dst in zip(refs[:3], refs[3:]):
        dst[...] = src[...]


def per_device(hidden_states, teacher_logits, head_weight):
    vmem = pl.BlockSpec(memory_space=pltpu.VMEM)
    hbm = pl.BlockSpec(memory_space=pl.ANY)
    kl, hidden_grad, head_grad = pl.pallas_call(
        kernel,
        out_shape=(
            jax.ShapeDtypeStruct((4, LANES), F32),
            jax.ShapeDtypeStruct((ROWS, PART), BF16),
            jax.ShapeDtypeStruct((64, VOCAB), F32),
        ),
        in_specs=[hbm, hbm, hbm],
        out_specs=(vmem, vmem, vmem),
        scratch_shapes=[pltpu.VMEM(*SCRATCH[k]) for k in NAMES]
        + [
            pltpu.SemaphoreType.DMA((10,)),
            pltpu.SemaphoreType.DMA((N_COPIES,)),
            pltpu.SemaphoreType.DMA((N_COPIES,)),
        ],
        compiler_params=pltpu.CompilerParams(
            collective_id=0, has_side_effects=True, vmem_limit_bytes=66_000_000
        ),
    )(hidden_states, teacher_logits, head_weight)
    kl, hidden_grad, head_grad = pl.pallas_call(
        handed_on,
        out_shape=tuple(jax.ShapeDtypeStruct(v.shape, v.dtype) for v in (kl, hidden_grad, head_grad)),
        in_specs=[vmem] * 3,
        out_specs=(vmem,) * 3,
    )(kl, hidden_grad, head_grad)
    return kl.reshape(ROWS), hidden_grad, head_grad


def solution(mesh):
    split = Mesh(mesh.devices.reshape(NY, NZ, NX, 2), ("y", "z", "x", "c"))
    dp, vocab = ("y", "z"), ("x", "c")
    return jax.shard_map(
        per_device,
        mesh=split,
        in_specs=(P(dp, vocab), P(dp, vocab), P(None, vocab)),
        out_specs=(P(dp), P(dp, vocab), P(dp, vocab)),
        check_vma=False,
    )
```

```python
import jax
import jax.numpy as jnp
from jax import lax
from jax.experimental import pallas as pl
from jax.experimental.pallas import tpu as pltpu
from jax.sharding import Mesh
from jax.sharding import PartitionSpec as P

MESH = pl.DeviceIdType.MESH
F32, BF16 = jnp.float32, jnp.bfloat16
NY, NZ, NX = 4, 8, 4
ROWS, WIDTH, VOCAB, PART = 512, 2048, 2048, 256
GRAD_SCALE = 8.0
LANES = 128

CHUNKS = tuple((k, 128) for k in "ZABaABBaAB")


def chunk_table():
    table, begin, half = [], 0, 0
    for kind, width in CHUNKS:
        paired = kind not in "Bb"
        table.append(dict(kind=kind.upper(), m=int(kind.islower()), w=width, paired=paired, at=begin, half=half))
        begin += width * (2 if paired else 1)
        half += width if paired else 0
    assert begin == VOCAB
    return table, half


TABLE, HALF_WIDTH = chunk_table()
EARLY = {("m", 0, "O"): 2.0, ("m", 1, "LR0"): 3.3, ("m", 1, "LR1"): 6.1}


def in_order(ops):
    rate = 46.0e3
    done, arrived, link_free, now, order = {}, dict(EARLY), {"x+": 2.9, "x-": 2.9}, 0.0, []
    left = list(ops)
    while left:
        best = None
        for rank, op in enumerate(left):
            if any(d not in done for d in op["after"]) or any(r not in arrived for r in op["recv"]):
                continue
            ready = max([now] + [arrived[r] for r in op["recv"]])
            key = (ready, op["rank"], rank)
            if best is None or key < best[0]:
                best = (key, op)
        (ready, _, _), op = best
        now = ready + op["time"]
        done[op["name"]] = now
        for link, size, key in op["send"]:
            begin = max(now, link_free.get(link, 0.0))
            wire = size / (rate if link != "c" else 600e3)
            link_free[link] = begin + wire
            arrived[key] = begin + wire + (2.8 if link != "c" else 1.0)
        order.append(op)
        left.remove(op)
    return order, now


def fold(op, tiles):
    tiles = list(tiles)
    while len(tiles) > 1:
        pairs = [op(a, b) for a, b in zip(tiles[::2], tiles[1::2])]
        tiles = pairs + ([tiles[-1]] if len(tiles) % 2 else [])
    return tiles[0]


def lane_tiles(value):
    return [value[:, i : i + LANES] for i in range(0, value.shape[1], LANES)]


SCRATCH = dict(
    hid=((8, ROWS, PART), BF16),
    hid_t=((3, NY, NZ, 64, ROWS), BF16),
    tea=((ROWS, VOCAB), BF16),
    head=((8, PART, VOCAB), BF16),
    stu=((ROWS, VOCAB), F32),
    stu_exp=((ROWS, VOCAB), F32),
    tea_exp=((ROWS, VOCAB), F32),
    grad=((ROWS, VOCAB), BF16),
    part_a=((ROWS, LANES), F32),
    part_b=((ROWS, LANES), F32),
    tea_max=((ROWS, LANES), F32),
    x_tea=((8, 8, LANES), F32),
    x_stu=((8, 8, LANES), F32),
    x_cross=((8, 8, LANES), F32),
    hid_m=((2, 8, ROWS, PART), BF16),
    grad_m=((ROWS, HALF_WIDTH), BF16),
    hs_s=((4, ROWS, PART), BF16),
    hs_r=((4, ROWS, PART), BF16),
    h1_s=((2, 256, PART), BF16),
    h1_r=((2, 256, PART), BF16),
    h2_s=((2, ROWS, PART), BF16),
    h2_r=((2, ROWS, PART), BF16),
)
for _i, _c in enumerate(TABLE):
    _w, _n = _c["w"], 2 if _c["kind"] == "A" else 4
    _cross = ROWS if _c["kind"] == "A" else 64
    for _side in "sr":
        SCRATCH[f"z1_{_side}{_i}"] = ((2, _n // 2, 64, _w), BF16)
        SCRATCH[f"z_{_side}{_i}"] = ((2, 3, _n, 64, _w), BF16)
        SCRATCH[f"x_{_side}{_i}"] = ((2, _cross, _w), BF16)
        SCRATCH[f"f_{_side}{_i}"] = ((64, _w), BF16)
    SCRATCH[f"z_sum{_i}"] = ((_n, 64, _w), F32)
    if _c["kind"] == "A":
        SCRATCH[f"a_sum{_i}"] = ((2, NZ, 64, _w), F32)
NAMES = tuple(SCRATCH)
N_COPIES = 200
WIDE = 1024


def kernel(hidden_in, teacher_in, head_in, kl_out, hg_out, gh_out, *rest):
    bufs = dict(zip(NAMES, rest))
    load_sem, send_sem, recv_sem = rest[len(NAMES) :]
    hid, hid_t, tea, head, stu = (bufs[k] for k in ("hid", "hid_t", "tea", "head", "stu"))
    stu_exp, tea_exp, grad = bufs["stu_exp"], bufs["tea_exp"], bufs["grad"]
    part_a, part_b, tea_max = bufs["part_a"], bufs["part_b"], bufs["tea_max"]

    y, z, x, c = (lax.axis_index(a) for a in ("y", "z", "x", "c"))

    def near(axis, delta):
        here, size = {"y": (y, NY), "z": (z, NZ), "x": (x, NX)}[axis]
        return lax.rem(here + (delta % size), size)

    def vocab_at(dx, dc):
        return 2 * near("x", dx) + (c if dc == 0 else 1 - c)

    me, sib = vocab_at(0, 0), vocab_at(0, 1)
    to_sib = {"c": 1 - c}
    peers = [(dx, dc) for dx in range(NX) for dc in range(2) if (dx, dc) != (0, 0)]

    def peer(dx, dc):
        return {"x": near("x", dx), "c": c if dc == 0 else 1 - c}

    numbers, sent = {}, []

    def remote(key, src, dst, device):
        number = numbers.setdefault(key, len(numbers))
        assert number < N_COPIES
        return pltpu.make_async_remote_copy(
            src_ref=src,
            dst_ref=dst,
            send_sem=send_sem.at[number],
            recv_sem=recv_sem.at[number],
            device_id=device,
            device_id_type=MESH,
        )

    def send(key, src, dst, device):
        copy = remote(key, src, dst, device)
        copy.start()
        sent.append(copy)

    def arrive(key, dst, device=None):
        remote(key, dst, dst, to_sib).wait_recv()

    loads = [pltpu.make_async_copy(hidden_in, hid.at[me], load_sem.at[0])]
    loads[0].start()
    slots = [vocab_at(*p) for p in ((0, 0), (0, 1), (3, 0), (1, 0), (3, 1), (1, 1), (2, 0), (2, 1))]
    own, sibling, left, right, left_s, right_s, far, far_s = slots
    head_loads = []
    for k, slot in enumerate(slots):
        rows = pl.ds(pl.multiple_of(slot * PART, PART), PART)
        head_loads.append(pltpu.make_async_copy(head_in.at[rows], head.at[slot], load_sem.at[1 + k]))
    tea_load = pltpu.make_async_copy(teacher_in, tea, load_sem.at[9])
    head_loads[0].start()
    head_loads[1].start()
    tea_load.start()
    for copy in head_loads[2:]:
        copy.start()

    barrier = pltpu.get_barrier_semaphore()
    around = [peer(*p) for p in peers] + [{a: near(a, d)} for a in "yz" for d in (1, -1)]
    for device in around:
        pl.semaphore_signal(barrier, inc=1, device_id=device, device_id_type=MESH)
    pl.semaphore_wait(barrier, len(around))

    halves = (pl.ds(0, 256), pl.ds(256, 256))
    x_right, x_left = {"x": near("x", 1)}, {"x": near("x", -1)}
    loads[0].wait()

    def half(slot, h):
        return hid.at[slot, halves[h]]

    def give(key, slot, h, device):
        send(key, half(slot, h), half(slot, h), device)

    give("L0", own, 0, x_right)
    give("R1", own, 1, x_left)
    send("own", hid.at[own], hid.at[own], to_sib)
    give("L1", own, 1, x_right)
    give("R0", own, 0, x_left)
    hid_m = bufs["hid_m"]
    rem2 = lax.rem(y, 2)
    partners = ({"y": y + 1 - 2 * rem2}, {"y": 3 - y})
    for m in range(2):
        send(("m", m, "y"), hid.at[own], hid_m.at[m, own], partners[m])

    def half_m(m, slot, h):
        return hid_m.at[m, slot, halves[h]]

    def give_m(m, key, slot, h, device):
        send(("m", m, key), half_m(m, slot, h), half_m(m, slot, h), device)

    def arrive_m(m, key, slot, h):
        arrive(("m", m, key), half_m(m, slot, h))

    def first_m(m):
        arrive(("m", m, "y"), hid_m.at[m, own])
        give_m(m, "L0", own, 0, x_right)
        give_m(m, "R1", own, 1, x_left)
        send(("m", m, "own"), hid_m.at[m, own], hid_m.at[m, own], to_sib)
        give_m(m, "L1", own, 1, x_right)
        give_m(m, "R0", own, 0, x_left)

    def second_m(m):
        arrive_m(m, "L0", left, 0)
        give_m(m, "O0", left, 0, x_right)
        give_m(m, "SL0", left, 0, to_sib)
        arrive_m(m, "R1", right, 1)
        give_m(m, "O1", right, 1, x_left)
        give_m(m, "SR1", right, 1, to_sib)

    def third_m(m):
        arrive_m(m, "L1", left, 1)
        give_m(m, "SL1", left, 1, to_sib)
        arrive_m(m, "R0", right, 0)
        give_m(m, "SR0", right, 0, to_sib)

    def fourth_m(m):
        for h in range(2):
            arrive_m(m, f"O{h}", far, h)
            give_m(m, f"SO{h}", far, h, to_sib)

    def turn(which, source):
        @pl.loop(0, NY)
        def _(j):
            for u in range(2):
                for b in range(4):
                    rows = slice(b * LANES, (b + 1) * LANES)
                    turned = source(2 * j + u, rows).T
                    hid_t[which, j, 4 * u : 4 * u + 4, :, rows] = turned.reshape(4, 64, LANES)

    def fifth_m(m):
        arrive(("m", m, "own"), hid_m.at[m, sibling])
        for h in range(2):
            arrive_m(m, f"SL{h}", left_s, h)
            arrive_m(m, f"SR{h}", right_s, h)
            arrive_m(m, f"SO{h}", far_s, h)
        turn(1 + m, lambda slot, rows: hid_m[m, slot, rows, :])

    def logits(ks, first=False):
        for k in ks:
            head_loads[k].wait()

        @pl.loop(0, VOCAB // WIDE)
        def _(n):
            cols = pl.ds(pl.multiple_of(n * WIDE, WIDE), WIDE)
            value = sum(
                jnp.dot(hid[slots[k]], head[slots[k], :, cols], preferred_element_type=F32) for k in ks
            )
            if first:
                stu[:, cols] = value
            else:
                stu[:, cols] += value

    def row_blocks(size, body):
        @pl.loop(0, ROWS // size)
        def _(n):
            body(pl.ds(pl.multiple_of(n * size, size), size))

    def spread_max(ref_in, ref_out):
        ref_out[...] = jnp.broadcast_to(jnp.max(ref_in[...], axis=1, keepdims=True), (ROWS, LANES))

    def tea_peaks(rows):
        part_a[rows, :] = fold(jnp.maximum, lane_tiles(tea[rows, :].astype(F32)))

    def tea_terms(rows):
        peak = tea_max[rows, :]
        total = None
        for i in range(0, VOCAB, LANES):
            term = jnp.exp(tea[rows, i : i + LANES].astype(F32) - peak)
            tea_exp[rows, i : i + LANES] = term
            total = term if total is None else total + term
        part_b[rows, :] = total

    def compact(ref, slot, at, peaks_ref):
        for b in range(4):
            rows = slice(b * LANES, (b + 1) * LANES)
            if peaks_ref is not None:
                ref[slot, b : b + 1, :] = peaks_ref[rows, :].T[0:1, :]
            ref[slot, at + b : at + b + 1, :] = jnp.sum(part_b[rows, :].T, axis=0, keepdims=True)

    def share(name):
        ref = bufs[name]
        for dx, dc in peers:
            send((name, dx, dc), ref.at[me], ref.at[me], peer(dx, dc))

    def shared(name):
        ref = bufs[name]
        for dx, dc in peers:
            slot = vocab_at(-dx, dc)
            arrive((name, dx, dc), ref.at[slot])

    def merged(ref):
        peak = fold(jnp.maximum, [ref[k, 0:4, :] for k in range(8)])
        total = None
        for k in range(8):
            term = ref[k, 4:8, :] * jnp.exp(ref[k, 0:4, :] - peak)
            total = term if total is None else total + term
        return peak, total

    def spread(value, ref):
        for b in range(4):
            ref[b * LANES : (b + 1) * LANES, :] = jnp.broadcast_to(
                value[b : b + 1, :], (LANES, LANES)
            ).T

    arrive("own", hid.at[sibling])
    logits((0, 1), first=True)
    tea_load.wait()
    row_blocks(32, tea_peaks)
    spread_max(part_a, tea_max)
    arrive("L0", half(left, 0))
    give("O0", left, 0, x_right)
    give("SL0", left, 0, to_sib)
    arrive("R1", half(right, 1))
    give("O1", right, 1, x_left)
    give("SR1", right, 1, to_sib)
    row_blocks(16, tea_terms)
    arrive("L1", half(left, 1))
    give("SL1", left, 1, to_sib)
    arrive("R0", half(right, 0))
    give("SR0", right, 0, to_sib)
    compact(bufs["x_tea"], me, 4, tea_max)
    share("x_tea")
    first_m(0)
    logits((2, 3))
    arrive("O0", half(far, 0))
    give("SO0", far, 0, to_sib)
    arrive("O1", half(far, 1))
    give("SO1", far, 1, to_sib)
    arrive("SL0", half(left_s, 0))
    arrive("SL1", half(left_s, 1))
    arrive("SR0", half(right_s, 0))
    arrive("SR1", half(right_s, 1))
    logits((4, 5))
    arrive("SO0", half(far_s, 0))
    arrive("SO1", half(far_s, 1))
    logits((6, 7))

    def stu_peaks(rows):
        part_a[rows, :] = fold(jnp.maximum, lane_tiles(stu[rows, :]))

    def stu_terms(rows):
        peak = part_a[rows, :]
        total = None
        for i in range(0, VOCAB, LANES):
            term = jnp.exp(stu[rows, i : i + LANES] - peak)
            stu_exp[rows, i : i + LANES] = term
            total = term if total is None else total + term
        part_b[rows, :] = total

    row_blocks(32, stu_peaks)
    spread_max(part_a, part_a)
    row_blocks(16, stu_terms)
    compact(bufs["x_stu"], me, 4, part_a)
    share("x_stu")

    turn(0, lambda slot, rows: hid[slot, rows, :])

    shared("x_tea")
    tea_peak, tea_total = merged(bufs["x_tea"])
    spread(GRAD_SCALE * jnp.exp(bufs["x_tea"][me, 0:4, :] - tea_peak) / tea_total, part_b)
    second_m(0)
    third_m(0)
    first_m(1)
    shared("x_stu")
    stu_peak, stu_total = merged(bufs["x_stu"])
    spread(GRAD_SCALE * jnp.exp(bufs["x_stu"][me, 0:4, :] - stu_peak) / stu_total, part_a)

    def grads(rows):
        stu_scale, tea_scale = part_a[rows, :], part_b[rows, :]
        for i in range(0, VOCAB, LANES):
            cols = slice(i, i + LANES)
            grad[rows, cols] = (stu_exp[rows, cols] * stu_scale - tea_exp[rows, cols] * tea_scale).astype(BF16)

    row_blocks(16, grads)

    ops = []

    def op(name, emit, time, rank, recv=(), send=(), after=()):
        ops.append(
            dict(name=name, emit=emit, time=time, rank=rank, recv=list(recv), send=list(send), after=list(after))
        )

    links = {("y", 0): "y+", ("y", 1): "y-", ("z", 0): "z+", ("z", 1): "z-", ("x", 0): "x+", ("x", 1): "x-"}

    def toward(axis, d):
        return {axis: near(axis, 1 if d == 0 else -1)}

    def signed(d, n):
        return n if d == 0 else -n

    grad_m = bufs["grad_m"]
    high = (y * (3 - y), y - rem2)

    op("g0o", lambda: fourth_m(0), 0.01, -3, recv=[("m", 0, "O")], send=[("c", 262144, ("m", 0, "SO"))])
    op("g0t", lambda: fifth_m(0), 0.78, -2, recv=[("m", 0, "SO")])
    op(
        "g1a",
        lambda: second_m(1),
        0.01,
        -3,
        recv=[("m", 1, "LR0")],
        send=[("x+", 131072, ("m", 1, "O0")), ("x-", 131072, ("m", 1, "O1")), ("c", 262144, ("m", 1, "S0"))],
    )
    op("g1b", lambda: third_m(1), 0.01, -3, recv=[("m", 1, "LR1")], send=[("c", 262144, ("m", 1, "S1"))], after=["g1a"])
    op(
        "g1o",
        lambda: fourth_m(1),
        0.01,
        -3,
        recv=[("m", 1, "O0"), ("m", 1, "O1")],
        send=[("c", 262144, ("m", 1, "SO"))],
        after=["g1b"],
    )
    op("g1t", lambda: fifth_m(1), 0.78, -2, recv=[("m", 1, k) for k in ("SO", "S0", "S1")])

    def chunk(i):
        info = TABLE[i]
        kind, m, w, paired, at, half_at = (info[k] for k in ("kind", "m", "w", "paired", "at", "half"))
        rank = 0.01 * i
        pair_link, cross_link = ("p", "q") if m == 0 else ("q", "p")
        partner, cross = partners[m], partners[1 - m]
        opposite = lax.rem(y + 2, NY)
        mine = pl.ds(pl.multiple_of(at + high[m] * (w // 2), LANES), w) if paired else pl.ds(at, w)
        theirs = pl.ds(pl.multiple_of(at + (2 - high[m]) * (w // 2), LANES), w) if paired else None
        got_cols = pl.ds(half_at, w)
        n = 2 if kind == "A" else 4
        z1_s, z1_r, z_s, z_r = (bufs[f"{k}{i}"] for k in ("z1_s", "z1_r", "z_s", "z_r"))
        x_s, x_r, f_s, f_r = (bufs[f"{k}{i}"] for k in ("x_s", "x_r", "f_s", "f_r"))
        z_sum = bufs[f"z_sum{i}"]

        def formed(rows_of):
            value = jnp.dot(rows_of(0), grad[:, mine], preferred_element_type=F32)
            if paired:
                value = value + jnp.dot(rows_of(1 + m), grad_m[:, got_cols], preferred_element_type=F32)
            return value

        def cost(rows):
            if kind == "A":
                return 0.71 if w == 128 else 1.1
            return ((0.3 if paired else 0.24) if rows == 256 else (0.22 if paired else 0.19)) * (1 if w == 128 else 1.5)

        start = []
        if paired:

            def emit_swap():
                send(("p", i), grad.at[:, theirs], grad_m.at[:, got_cols], partner)

            def emit_swapped():
                arrive(("p", i), grad_m.at[:, got_cols])

            op(("p", i), emit_swap, 0.02, -1 + rank, send=[(pair_link, 1024 * w, ("p", i))])
            op(("pr", i), emit_swapped, 0.01, rank, recv=[("p", i)], after=[f"g{m}t"])
            start = [("pr", i)]

        if kind == "A":
            a_sum = bufs[f"a_sum{i}"]

            def emit_cross():
                for u, j in enumerate((cross["y"], opposite)):
                    x_s[u] = formed(lambda t: hid_t[t, j].reshape(ROWS, ROWS)).astype(BF16)
                send(("q", i), x_s, x_r, cross)

            def emit_kept():
                arrive(("q", i), x_r)
                for u, j in enumerate((y, partner["y"])):
                    value = formed(lambda t: hid_t[t, j].reshape(ROWS, ROWS)) + x_r[u].astype(F32)
                    a_sum[u] = value.reshape(NZ, 64, w)

            op(("q", i), emit_cross, cost(1024), rank, send=[(cross_link, 2048 * w, ("q", i))], after=start)
            op(("qf", i), emit_kept, cost(1024), rank, recv=[("q", i)], after=start)
            start = [("qf", i)]

        def z_part(k, lo, count):
            if kind == "A":
                return a_sum[lo : lo + count, near("z", k)]
            value = formed(lambda t: hid_t[t, lo : lo + count, near("z", k)].reshape(64 * count, ROWS))
            return value.reshape(count, 64, w)

        h = n // 2

        def z_step(d, step):
            dest = signed(d, 5 - step)
            lo = d * h
            src, dst = (z1_s.at[d], z1_r.at[d]) if step == 1 else (z_s.at[d, step - 2], z_r.at[d, step - 2])

            def emit():
                if step == 1:
                    z1_s[d] = z_part(dest, lo, h).astype(BF16)
                elif step == 2:
                    arrive(("z", i, d, 1), z1_r.at[d])
                    z_s[d, 0, h - lo : n - lo] = z_part(dest, h - lo, h).astype(BF16)
                    z_s[d, 0, lo : lo + h] = (z_part(dest, lo, h) + z1_r[d].astype(F32)).astype(BF16)
                else:
                    arrive(("z", i, d, step - 1), z_r.at[d, step - 3])
                    z_s[d, step - 2] = (z_part(dest, 0, n) + z_r[d, step - 3].astype(F32)).astype(BF16)
                send(("z", i, d, step), src, dst, toward("z", d))

            time = 0.012 if kind == "A" else cost(128 if step == 1 else 256)
            op(
                ("z", i, d, step),
                emit,
                time,
                rank + (0.5 if step == 1 else 0),
                recv=[("z", i, d, step - 1)] if step > 1 else [],
                send=[(links["z", d], 128 * w * (h if step == 1 else n), ("z", i, d, step))],
                after=start,
            )

        def emit_z_last():
            for d in range(2):
                arrive(("z", i, d, 4), z_r.at[d, 2])
            z_sum[...] = z_part(0, 0, n) + z_r[0, 2].astype(F32) + z_r[1, 2].astype(F32)

        def finish(kept, other):
            f_s[...] = other.astype(BF16)
            send(("f", i), f_s, f_r, partner)
            if paired:
                gh_out[:, mine] = kept
            else:
                z_sum[0] = kept

        def emit_last():
            arrive(("f", i), f_r)
            if paired:
                gh_out[:, theirs] = f_r[...].astype(F32)
            else:
                gh_out[:, mine] = z_sum[0] + f_r[...].astype(F32)

        for d in range(2):
            for step in range(1, 5):
                z_step(d, step)
        op(("zf", i), emit_z_last, 0.012 if kind == "A" else cost(256), rank, recv=[("z", i, d, 4) for d in range(2)], after=start)
        final = [(pair_link, 128 * w, ("f", i))]
        if kind == "A":
            op(("fs", i), lambda: finish(z_sum[0], z_sum[1]), 0.02, rank, send=final, after=[("zf", i)])
            op(("ff", i), emit_last, 0.02, rank, recv=[("f", i)], after=[("fs", i)])
        else:

            def emit_cross_small():
                for u, j in enumerate((cross["y"], opposite)):
                    x_s[u] = z_sum[j].astype(BF16)
                send(("q", i), x_s, x_r, cross)

            def emit_kept_small():
                arrive(("q", i), x_r)
                finish(z_sum[y] + x_r[0].astype(F32), z_sum[partner["y"]] + x_r[1].astype(F32))

            op(("q", i), emit_cross_small, 0.02, rank, send=[(cross_link, 256 * w, ("q", i))], after=[("zf", i)])
            op(("qf", i), emit_kept_small, 0.02, rank, recv=[("q", i)], send=final, after=[("q", i)])
            op(("ff", i), emit_last, 0.02, rank, recv=[("f", i)], after=[("qf", i)])

    for i in range(len(TABLE)):
        chunk(i)

    hops = (2, 1, 3, 0)

    def back(slot, h):
        return lax.dot_general(
            grad[halves[h], :], head[slot], (((1,), (1,)), ((), ())), preferred_element_type=F32
        )

    def hs_step(n):
        def emit():
            slot = vocab_at(hops[n], 1)
            for h in range(2):
                bufs["hs_s"][n, halves[h], :] = back(slot, h).astype(BF16)
            send(("hs", n), bufs["hs_s"].at[n], bufs["hs_r"].at[n], to_sib)

        op(("hs", n), emit, 0.76, 3, send=[("c", 262144, ("hs", n))])

    def hg_step(n):
        def emit():
            arrive(("hs", n), bufs["hs_r"].at[n])
            if n == 1 or n == 2:
                d = n - 1
                arrive(("h1", d), bufs["h1_r"].at[d])
            if n == 3:
                for d in range(2):
                    arrive(("h2", d), bufs["h2_r"].at[d])
            slot = vocab_at(hops[n], 0)
            for h in range(2):
                rows = halves[h]
                value = back(slot, h) + bufs["hs_r"][n, rows, :].astype(F32)
                if n == 0:
                    bufs["h1_s"][h] = value.astype(BF16)
                    send(("h1", h), bufs["h1_s"].at[h], bufs["h1_r"].at[h], toward("x", h))
                elif n < 3:
                    if h == n - 1:
                        value = value + bufs["h1_r"][h].astype(F32)
                    bufs["h2_s"][n - 1, rows, :] = value.astype(BF16)
                else:
                    got = [bufs["h2_r"][d, rows, :].astype(F32) for d in range(2)]
                    hg_out[rows, :] = (value + got[0] + got[1]).astype(BF16)
            if n == 1 or n == 2:
                d = n - 1
                send(("h2", d), bufs["h2_s"].at[d], bufs["h2_r"].at[d], toward("x", d))

        recv = [("hs", n)] + {0: [], 1: [("h1", 0)], 2: [("h1", 1)], 3: [("h2", 0), ("h2", 1)]}[n]
        sends = {
            0: [("x+", 131072, ("h1", 0)), ("x-", 131072, ("h1", 1))],
            1: [("x+", 262144, ("h2", 0))],
            2: [("x-", 262144, ("h2", 1))],
            3: [],
        }[n]
        op(("hg", n), emit, 0.77 if n else 1.45, 3, recv=recv, send=sends)

    for n in range(4):
        hs_step(n)
        hg_step(n)

    def cross_share():
        def emit():
            def terms(rows):
                total = None
                for i in range(0, VOCAB, LANES):
                    cols = slice(i, i + LANES)
                    term = tea_exp[rows, cols] * (tea[rows, cols].astype(F32) - stu[rows, cols])
                    total = term if total is None else total + term
                part_b[rows, :] = total

            row_blocks(16, terms)
            ref = bufs["x_cross"]
            ref[me, 4:8, :] = jnp.zeros((4, LANES), F32)
            compact(ref, me, 0, None)
            share("x_cross")

        op("cross", emit, 1.06, 4)

    def divergence():
        def emit():
            shared("x_cross")
            ref, peaks = bufs["x_cross"], bufs["x_tea"]
            peak, total = merged(peaks)
            s_peak, s_total = merged(bufs["x_stu"])
            cross = None
            for k in range(8):
                term = ref[k, 0:4, :] * jnp.exp(peaks[k, 0:4, :] - peak)
                cross = term if cross is None else cross + term
            kl_out[...] = cross / total - peak - jnp.log(total) + s_peak + jnp.log(s_total)

        op("kl", emit, 0.05, 5, after=["cross", ("hg", 3)])

    cross_share()
    divergence()

    order, _ = in_order(ops)
    for step in order:
        step["emit"]()

    for copy in sent:
        copy.wait_send()


def handed_on(*refs):
    for src, dst in zip(refs[:3], refs[3:]):
        dst[...] = src[...]


def per_device(hidden_states, teacher_logits, head_weight):
    vmem = pl.BlockSpec(memory_space=pltpu.VMEM)
    hbm = pl.BlockSpec(memory_space=pl.ANY)
    kl, hidden_grad, head_grad = pl.pallas_call(
        kernel,
        out_shape=(
            jax.ShapeDtypeStruct((4, LANES), F32),
            jax.ShapeDtypeStruct((ROWS, PART), BF16),
            jax.ShapeDtypeStruct((64, VOCAB), F32),
        ),
        in_specs=[hbm, hbm, hbm],
        out_specs=(vmem, vmem, vmem),
        scratch_shapes=[pltpu.VMEM(*SCRATCH[k]) for k in NAMES]
        + [
            pltpu.SemaphoreType.DMA((10,)),
            pltpu.SemaphoreType.DMA((N_COPIES,)),
            pltpu.SemaphoreType.DMA((N_COPIES,)),
        ],
        compiler_params=pltpu.CompilerParams(
            collective_id=0, has_side_effects=True, vmem_limit_bytes=66_000_000
        ),
    )(hidden_states, teacher_logits, head_weight)
    kl, hidden_grad, head_grad = pl.pallas_call(
        handed_on,
        out_shape=tuple(jax.ShapeDtypeStruct(v.shape, v.dtype) for v in (kl, hidden_grad, head_grad)),
        in_specs=[vmem] * 3,
        out_specs=(vmem,) * 3,
    )(kl, hidden_grad, head_grad)
    return kl.reshape(ROWS), hidden_grad, head_grad


def solution(mesh):
    split = Mesh(mesh.devices.reshape(NY, NZ, NX, 2), ("y", "z", "x", "c"))
    dp, vocab = ("y", "z"), ("x", "c")
    return jax.shard_map(
        per_device,
        mesh=split,
        in_specs=(P(dp, vocab), P(dp, vocab), P(None, vocab)),
        out_specs=(P(dp), P(dp, vocab), P(dp, vocab)),
        check_vma=False,
    )
```

```python
import jax
import jax.numpy as jnp
from jax import lax
from jax.experimental import pallas as pl
from jax.experimental.pallas import tpu as pltpu
from jax.sharding import Mesh
from jax.sharding import PartitionSpec as P

MESH = pl.DeviceIdType.MESH
F32, BF16 = jnp.float32, jnp.bfloat16
NY, NZ, NX = 4, 8, 4
ROWS, WIDTH, VOCAB, PART = 512, 2048, 2048, 256
GRAD_SCALE = 8.0
LANES = 128

CHUNKS = tuple((k, 128) for k in "ZAabAbbbAa")
RANKS = (0.8, 6.2, 8.9, 2.0, 9.1, 6.0, 6.7, 2.5, 8.9, 6.5)
SWAPS = (1, 2, 9, 3, 7, 6, 5, 4, 0, 8)
FIRST = -3


def chunk_table():
    table, begin, half = [], 0, 0
    for (kind, width), rank, turn in zip(CHUNKS, RANKS, SWAPS):
        paired = kind not in "Bb"
        table.append(dict(kind=kind.upper(), m=int(kind.islower()), w=width, paired=paired, at=begin, half=half, rank=rank, turn=turn))
        begin += width * (2 if paired else 1)
        half += width if paired else 0
    assert begin == VOCAB
    return table, half


TABLE, HALF_WIDTH = chunk_table()
EARLY = {("m", 0, "O"): 2.0, ("m", 1, "LR0"): 3.3, ("m", 1, "LR1"): 6.1}


RATE = 46.0e3


def in_order(ops):
    done, arrived, link_free, now, order = {}, dict(EARLY), {"x+": 2.9, "x-": 2.9}, 0.0, []
    left = list(ops)
    while left:
        best = None
        for rank, op in enumerate(left):
            if any(d not in done for d in op["after"]) or any(r not in arrived for r in op["recv"]):
                continue
            ready = max([now] + [arrived[r] for r in op["recv"]])
            key = (ready, op["rank"], rank)
            if best is None or key < best[0]:
                best = (key, op)
        (ready, _, _), op = best
        now = ready + op["time"]
        done[op["name"]] = now
        for link, size, key in op["send"]:
            begin = max(now, link_free.get(link, 0.0))
            wire = size / (RATE if link != "c" else 600e3)
            link_free[link] = begin + wire
            hops = 0.75 if link[0] == "z" and key[0] == "f" or link[0] in "pq" and key[0] == "f" and key[2] == 2 else 0.0
            arrived[key] = begin + wire + (2.8 + hops if link != "c" else 1.0)
        order.append(op)
        left.remove(op)
    return order, now


def fold(op, tiles):
    tiles = list(tiles)
    while len(tiles) > 1:
        pairs = [op(a, b) for a, b in zip(tiles[::2], tiles[1::2])]
        tiles = pairs + ([tiles[-1]] if len(tiles) % 2 else [])
    return tiles[0]


def lane_tiles(value):
    return [value[:, i : i + LANES] for i in range(0, value.shape[1], LANES)]


SCRATCH = dict(
    hid=((8, ROWS, PART), BF16),
    hid_t=((3, NY, NZ, 64, ROWS), BF16),
    tea=((ROWS, VOCAB), BF16),
    head=((8, PART, VOCAB), BF16),
    stu=((ROWS, VOCAB), F32),
    stu_exp=((ROWS, VOCAB), F32),
    tea_exp=((ROWS, VOCAB), F32),
    grad=((ROWS, VOCAB), BF16),
    part_a=((ROWS, LANES), F32),
    part_b=((ROWS, LANES), F32),
    part_c=((ROWS, LANES), F32),
    tea_max=((ROWS, LANES), F32),
    x_tea=((8, 8, LANES), F32),
    x_stu=((8, 8, LANES), F32),
    x_cross=((8, 8, LANES), F32),
    hid_m=((2, 8, ROWS, PART), BF16),
    grad_m=((ROWS, HALF_WIDTH), BF16),
    hs_s=((4, ROWS, PART), BF16),
    hs_r=((4, ROWS, PART), BF16),
    h1_s=((2, 256, PART), BF16),
    h1_r=((2, 256, PART), BF16),
    h2_s=((2, ROWS, PART), BF16),
    h2_r=((2, ROWS, PART), BF16),
)
for _i, _c in enumerate(TABLE):
    _w, _n = _c["w"], 2 if _c["kind"] == "A" else 4
    for _side in "sr":
        SCRATCH[f"z1_{_side}{_i}"] = ((2, _n // 2, 64, _w), BF16)
        SCRATCH[f"z_{_side}{_i}"] = ((2, 3, _n, 64, _w), BF16)
        SCRATCH[f"f_{_side}{_i}"] = ((3, 64, _w), BF16)
        if _c["kind"] == "A":
            SCRATCH[f"x_{_side}{_i}"] = ((2, ROWS, _w), BF16)
    if _c["kind"] == "A":
        SCRATCH[f"a_sum{_i}"] = ((2, NZ, 64, _w), F32)
    else:
        SCRATCH[f"z_sum{_i}"] = ((4, 64, _w), F32)
NAMES = tuple(SCRATCH)
N_COPIES = 230
WIDE = 1024


def kernel(hidden_in, teacher_in, head_in, kl_out, hg_out, gh_out, *rest):
    bufs = dict(zip(NAMES, rest))
    load_sem, send_sem, recv_sem = rest[len(NAMES) :]
    hid, hid_t, tea, head, stu = (bufs[k] for k in ("hid", "hid_t", "tea", "head", "stu"))
    stu_exp, tea_exp, grad = bufs["stu_exp"], bufs["tea_exp"], bufs["grad"]
    part_a, part_b, tea_max = bufs["part_a"], bufs["part_b"], bufs["tea_max"]

    y, z, x, c = (lax.axis_index(a) for a in ("y", "z", "x", "c"))

    def near(axis, delta):
        here, size = {"y": (y, NY), "z": (z, NZ), "x": (x, NX)}[axis]
        return lax.rem(here + (delta % size), size)

    def vocab_at(dx, dc):
        return 2 * near("x", dx) + (c if dc == 0 else 1 - c)

    me, sib = vocab_at(0, 0), vocab_at(0, 1)
    to_sib = {"c": 1 - c}
    peers = [(dx, dc) for dx in range(NX) for dc in range(2) if (dx, dc) != (0, 0)]

    def peer(dx, dc):
        return {"x": near("x", dx), "c": c if dc == 0 else 1 - c}

    numbers, sent = {}, []

    def remote(key, src, dst, device):
        number = numbers.setdefault(key, len(numbers))
        assert number < N_COPIES
        return pltpu.make_async_remote_copy(
            src_ref=src,
            dst_ref=dst,
            send_sem=send_sem.at[number],
            recv_sem=recv_sem.at[number],
            device_id=device,
            device_id_type=MESH,
        )

    def send(key, src, dst, device):
        copy = remote(key, src, dst, device)
        copy.start()
        sent.append(copy)

    def arrive(key, dst, device=None):
        remote(key, dst, dst, to_sib).wait_recv()

    loads = [pltpu.make_async_copy(hidden_in, hid.at[me], load_sem.at[0])]
    loads[0].start()
    slots = [vocab_at(*p) for p in ((0, 0), (0, 1), (3, 0), (1, 0), (3, 1), (1, 1), (2, 0), (2, 1))]
    own, sibling, left, right, left_s, right_s, far, far_s = slots
    head_loads = []
    for k, slot in enumerate(slots):
        rows = pl.ds(pl.multiple_of(slot * PART, PART), PART)
        head_loads.append(pltpu.make_async_copy(head_in.at[rows], head.at[slot], load_sem.at[1 + k]))
    tea_load = pltpu.make_async_copy(teacher_in, tea, load_sem.at[9])
    head_loads[0].start()
    head_loads[1].start()
    tea_load.start()
    for copy in head_loads[2:]:
        copy.start()

    barrier = pltpu.get_barrier_semaphore()
    around = [peer(*p) for p in peers] + [{"y": near("y", d)} for d in (1, -1, 2)] + [{"z": near("z", d)} for d in (1, -1)]
    around += [{"y": near("y", d), "z": near("z", e)} for d in (1, -1) for e in (1, -1)]
    for device in around:
        pl.semaphore_signal(barrier, inc=1, device_id=device, device_id_type=MESH)
    pl.semaphore_wait(barrier, len(around))

    halves = (pl.ds(0, 256), pl.ds(256, 256))
    x_right, x_left = {"x": near("x", 1)}, {"x": near("x", -1)}
    loads[0].wait()

    def half(slot, h):
        return hid.at[slot, halves[h]]

    def give(key, slot, h, device):
        send(key, half(slot, h), half(slot, h), device)

    give("L0", own, 0, x_right)
    give("R1", own, 1, x_left)
    send("own", hid.at[own], hid.at[own], to_sib)
    give("L1", own, 1, x_right)
    give("R0", own, 0, x_left)
    hid_m = bufs["hid_m"]
    rem2 = lax.rem(y, 2)
    partners = ({"y": y + 1 - 2 * rem2}, {"y": 3 - y})
    for m in range(2):
        send(("m", m, "y"), hid.at[own], hid_m.at[m, own], partners[m])

    def half_m(m, slot, h):
        return hid_m.at[m, slot, halves[h]]

    def give_m(m, key, slot, h, device):
        send(("m", m, key), half_m(m, slot, h), half_m(m, slot, h), device)

    def arrive_m(m, key, slot, h):
        arrive(("m", m, key), half_m(m, slot, h))

    def first_m(m):
        arrive(("m", m, "y"), hid_m.at[m, own])
        give_m(m, "L0", own, 0, x_right)
        give_m(m, "R1", own, 1, x_left)
        send(("m", m, "own"), hid_m.at[m, own], hid_m.at[m, own], to_sib)
        give_m(m, "L1", own, 1, x_right)
        give_m(m, "R0", own, 0, x_left)

    def second_m(m):
        arrive_m(m, "L0", left, 0)
        give_m(m, "O0", left, 0, x_right)
        give_m(m, "SL0", left, 0, to_sib)
        arrive_m(m, "R1", right, 1)
        give_m(m, "O1", right, 1, x_left)
        give_m(m, "SR1", right, 1, to_sib)

    def third_m(m):
        arrive_m(m, "L1", left, 1)
        give_m(m, "SL1", left, 1, to_sib)
        arrive_m(m, "R0", right, 0)
        give_m(m, "SR0", right, 0, to_sib)

    def fourth_m(m):
        for h in range(2):
            arrive_m(m, f"O{h}", far, h)
            give_m(m, f"SO{h}", far, h, to_sib)

    def turn(which, source):
        @pl.loop(0, NY)
        def _(j):
            for u in range(2):
                for b in range(4):
                    rows = slice(b * LANES, (b + 1) * LANES)
                    turned = source(2 * j + u, rows).T
                    hid_t[which, j, 4 * u : 4 * u + 4, :, rows] = turned.reshape(4, 64, LANES)

    def fifth_m(m):
        arrive(("m", m, "own"), hid_m.at[m, sibling])
        for h in range(2):
            arrive_m(m, f"SL{h}", left_s, h)
            arrive_m(m, f"SR{h}", right_s, h)
            arrive_m(m, f"SO{h}", far_s, h)
        turn(1 + m, lambda slot, rows: hid_m[m, slot, rows, :])

    def logits(ks, first=False):
        for k in ks:
            head_loads[k].wait()

        @pl.loop(0, VOCAB // WIDE)
        def _(n):
            cols = pl.ds(pl.multiple_of(n * WIDE, WIDE), WIDE)
            value = sum(
                jnp.dot(hid[slots[k]], head[slots[k], :, cols], preferred_element_type=F32) for k in ks
            )
            if first:
                stu[:, cols] = value
            else:
                stu[:, cols] += value

    def row_blocks(size, body):
        @pl.loop(0, ROWS // size)
        def _(n):
            body(pl.ds(pl.multiple_of(n * size, size), size))

    def spread_max(ref_in, ref_out):
        ref_out[...] = jnp.broadcast_to(jnp.max(ref_in[...], axis=1, keepdims=True), (ROWS, LANES))

    def tea_peaks(rows):
        part_a[rows, :] = fold(jnp.maximum, lane_tiles(tea[rows, :].astype(F32)))

    def tea_terms(rows):
        peak = tea_max[rows, :]
        total = None
        for i in range(0, VOCAB, LANES):
            term = jnp.exp(tea[rows, i : i + LANES].astype(F32) - peak)
            tea_exp[rows, i : i + LANES] = term
            total = term if total is None else total + term
        part_b[rows, :] = total

    def compact(ref, slot, at, peaks_ref, sums_ref=part_b):
        for b in range(4):
            rows = slice(b * LANES, (b + 1) * LANES)
            if peaks_ref is not None:
                ref[slot, b : b + 1, :] = peaks_ref[rows, :].T[0:1, :]
            ref[slot, at + b : at + b + 1, :] = jnp.sum(sums_ref[rows, :].T, axis=0, keepdims=True)

    def share(name):
        ref = bufs[name]
        for dx, dc in peers:
            send((name, dx, dc), ref.at[me], ref.at[me], peer(dx, dc))

    def shared(name):
        ref = bufs[name]
        for dx, dc in peers:
            slot = vocab_at(-dx, dc)
            arrive((name, dx, dc), ref.at[slot])

    def merged(ref):
        peak = fold(jnp.maximum, [ref[k, 0:4, :] for k in range(8)])
        total = None
        for k in range(8):
            term = ref[k, 4:8, :] * jnp.exp(ref[k, 0:4, :] - peak)
            total = term if total is None else total + term
        return peak, total

    def spread(value, ref):
        for b in range(4):
            ref[b * LANES : (b + 1) * LANES, :] = jnp.broadcast_to(
                value[b : b + 1, :], (LANES, LANES)
            ).T

    arrive("own", hid.at[sibling])
    logits((0, 1), first=True)
    tea_load.wait()
    row_blocks(32, tea_peaks)
    spread_max(part_a, tea_max)
    arrive("L0", half(left, 0))
    give("O0", left, 0, x_right)
    give("SL0", left, 0, to_sib)
    arrive("R1", half(right, 1))
    give("O1", right, 1, x_left)
    give("SR1", right, 1, to_sib)
    row_blocks(16, tea_terms)
    arrive("L1", half(left, 1))
    give("SL1", left, 1, to_sib)
    arrive("R0", half(right, 0))
    give("SR0", right, 0, to_sib)
    compact(bufs["x_tea"], me, 4, tea_max)
    share("x_tea")
    first_m(0)
    logits((2, 3))
    arrive("SL0", half(left_s, 0))
    arrive("SL1", half(left_s, 1))
    arrive("SR0", half(right_s, 0))
    arrive("SR1", half(right_s, 1))
    logits((4, 5))
    arrive("O0", half(far, 0))
    give("SO0", far, 0, to_sib)
    arrive("O1", half(far, 1))
    give("SO1", far, 1, to_sib)
    logits((6,))
    arrive("SO0", half(far_s, 0))
    arrive("SO1", half(far_s, 1))
    logits((7,))

    def stu_peaks(rows):
        part_a[rows, :] = fold(jnp.maximum, lane_tiles(stu[rows, :]))

    def stu_terms(rows):
        peak = part_a[rows, :]
        total = None
        for i in range(0, VOCAB, LANES):
            term = jnp.exp(stu[rows, i : i + LANES] - peak)
            stu_exp[rows, i : i + LANES] = term
            total = term if total is None else total + term
        part_b[rows, :] = total

    def cross_terms(rows):
        total = None
        for i in range(0, VOCAB, LANES):
            cols = slice(i, i + LANES)
            term = tea_exp[rows, cols] * (tea[rows, cols].astype(F32) - stu[rows, cols])
            total = term if total is None else total + term
        bufs["part_c"][rows, :] = total

    row_blocks(32, stu_peaks)
    spread_max(part_a, part_a)
    row_blocks(16, stu_terms)
    compact(bufs["x_stu"], me, 4, part_a)
    share("x_stu")

    turn(0, lambda slot, rows: hid[slot, rows, :])

    shared("x_tea")
    tea_peak, tea_total = merged(bufs["x_tea"])
    spread(GRAD_SCALE * jnp.exp(bufs["x_tea"][me, 0:4, :] - tea_peak) / tea_total, part_b)
    second_m(0)
    third_m(0)
    first_m(1)
    row_blocks(16, cross_terms)
    bufs["x_cross"][me, 4:8, :] = jnp.zeros((4, LANES), F32)
    compact(bufs["x_cross"], me, 0, None, bufs["part_c"])
    share("x_cross")
    shared("x_stu")
    stu_peak, stu_total = merged(bufs["x_stu"])
    spread(GRAD_SCALE * jnp.exp(bufs["x_stu"][me, 0:4, :] - stu_peak) / stu_total, part_a)

    def grads(rows):
        stu_scale, tea_scale = part_a[rows, :], part_b[rows, :]
        for i in range(0, VOCAB, LANES):
            cols = slice(i, i + LANES)
            grad[rows, cols] = (stu_exp[rows, cols] * stu_scale - tea_exp[rows, cols] * tea_scale).astype(BF16)

    row_blocks(16, grads)

    ops = []

    def op(name, emit, time, rank, recv=(), send=(), after=()):
        ops.append(
            dict(name=name, emit=emit, time=time, rank=rank, recv=list(recv), send=list(send), after=list(after))
        )

    links = {("y", 0): "y+", ("y", 1): "y-", ("z", 0): "z+", ("z", 1): "z-", ("x", 0): "x+", ("x", 1): "x-"}

    def toward(axis, d):
        return {axis: near(axis, 1 if d == 0 else -1)}

    def signed(d, n):
        return n if d == 0 else -n

    grad_m = bufs["grad_m"]
    high = (y * (3 - y), y - rem2)

    op("g0o", lambda: fourth_m(0), 0.01, -5, recv=[("m", 0, "O")], send=[("c", 262144, ("m", 0, "SO"))])
    op("g0t", lambda: fifth_m(0), 0.78, -5, recv=[("m", 0, "SO")])
    op(
        "g1a",
        lambda: second_m(1),
        0.01,
        -3,
        recv=[("m", 1, "LR0")],
        send=[("x+", 131072, ("m", 1, "O0")), ("x-", 131072, ("m", 1, "O1")), ("c", 262144, ("m", 1, "S0"))],
    )
    op("g1b", lambda: third_m(1), 0.01, -3, recv=[("m", 1, "LR1")], send=[("c", 262144, ("m", 1, "S1"))], after=["g1a"])
    op(
        "g1o",
        lambda: fourth_m(1),
        0.01,
        -3,
        recv=[("m", 1, "O0"), ("m", 1, "O1")],
        send=[("c", 262144, ("m", 1, "SO"))],
        after=["g1b"],
    )
    op("g1t", lambda: fifth_m(1), 0.78, -5, recv=[("m", 1, k) for k in ("SO", "S0", "S1")])

    def chunk(i):
        info = TABLE[i]
        kind, m, w, paired, at, half_at = (info[k] for k in ("kind", "m", "w", "paired", "at", "half"))
        rank = info["rank"]
        pair_link, cross_link = ("p", "q") if m == 0 else ("q", "p")
        partner, cross = partners[m], partners[1 - m]
        opposite = lax.rem(y + 2, NY)
        mine = pl.ds(pl.multiple_of(at + high[m] * (w // 2), LANES), w) if paired else pl.ds(at, w)
        theirs = pl.ds(pl.multiple_of(at + (2 - high[m]) * (w // 2), LANES), w) if paired else None
        got_cols = pl.ds(half_at, w)
        n = 2 if kind == "A" else 4
        z1_s, z1_r, z_s, z_r = (bufs[f"{k}{i}"] for k in ("z1_s", "z1_r", "z_s", "z_r"))
        f_s, f_r = (bufs[f"{k}{i}"] for k in ("f_s", "f_r"))

        def formed(rows_of):
            value = jnp.dot(rows_of(0), grad[:, mine], preferred_element_type=F32)
            if paired:
                value = value + jnp.dot(rows_of(1 + m), grad_m[:, got_cols], preferred_element_type=F32)
            return value

        def cost(rows):
            if kind == "A":
                return 0.71 if w == 128 else 1.1
            return ((0.3 if paired else 0.24) if rows == 256 else (0.22 if paired else 0.19)) * (1 if w == 128 else 1.5)

        start = []
        if paired:

            def emit_swap():
                send(("p", i), grad.at[:, theirs], grad_m.at[:, got_cols], partner)

            def emit_swapped():
                arrive(("p", i), grad_m.at[:, got_cols])

            op(("p", i), emit_swap, 0.02, -10 + 0.01 * info["turn"], send=[(pair_link, 1024 * w, ("p", i))])
            op(("pr", i), emit_swapped, 0.01, rank, recv=[("p", i)], after=[f"g{m}t"])
            start = [("pr", i)]

        if kind == "A":
            a_sum, x_s, x_r = (bufs[f"{k}{i}"] for k in ("a_sum", "x_s", "x_r"))

            def emit_cross():
                for u, j in enumerate((cross["y"], opposite)):
                    x_s[u] = formed(lambda t: hid_t[t, j].reshape(ROWS, ROWS)).astype(BF16)
                send(("q", i), x_s, x_r, cross)

            def emit_kept():
                arrive(("q", i), x_r)
                for u, j in enumerate((y, partner["y"])):
                    value = formed(lambda t: hid_t[t, j].reshape(ROWS, ROWS)) + x_r[u].astype(F32)
                    a_sum[u] = value.reshape(NZ, 64, w)
                f_s[0] = a_sum[1, z].astype(BF16)
                send(("f", i, 0), f_s.at[0], f_r.at[0], partner)

            op(("q", i), emit_cross, cost(1024), rank, send=[(cross_link, 2048 * w, ("q", i))], after=start)
            op(
                ("qf", i),
                emit_kept,
                cost(1024),
                rank,
                recv=[("q", i)],
                send=[(pair_link, 128 * w, ("f", i, 0))],
                after=start,
            )
            start = [("qf", i)]

        def z_part(k, lo, count):
            if kind == "A":
                return a_sum[lo : lo + count, near("z", k)]
            value = formed(lambda t: hid_t[t, lo : lo + count, near("z", k)].reshape(64 * count, ROWS))
            return value.reshape(count, 64, w)

        h = n // 2

        def z_step(d, step):
            dest = signed(d, 5 - step)
            lo = d * h
            src, dst = (z1_s.at[d], z1_r.at[d]) if step == 1 else (z_s.at[d, step - 2], z_r.at[d, step - 2])

            def emit():
                if step == 1:
                    z1_s[d] = z_part(dest, lo, h).astype(BF16)
                elif step == 2:
                    arrive(("z", i, d, 1), z1_r.at[d])
                    z_s[d, 0, h - lo : n - lo] = z_part(dest, h - lo, h).astype(BF16)
                    z_s[d, 0, lo : lo + h] = (z_part(dest, lo, h) + z1_r[d].astype(F32)).astype(BF16)
                else:
                    arrive(("z", i, d, step - 1), z_r.at[d, step - 3])
                    z_s[d, step - 2] = (z_part(dest, 0, n) + z_r[d, step - 3].astype(F32)).astype(BF16)
                if kind == "A" and step == 4:
                    send(("z", i, d, 4), src.at[0], dst.at[0], toward("z", d))
                    send(("f", i, 1 + d), src.at[1], f_r.at[1 + d], {**partner, **toward("z", d)})
                else:
                    send(("z", i, d, step), src, dst, toward("z", d))

            time = 0.012 if kind == "A" else cost(128 if step == 1 else 256)
            alone = kind == "A" and step == 4
            op(
                ("z", i, d, step),
                emit,
                time,
                rank + (FIRST if step == 1 else 0),
                recv=[("z", i, d, step - 1)] if step > 1 else [],
                send=[(links["z", d], 128 * w * (1 if alone else h if step == 1 else n), ("z", i, d, step))]
                + ([(links["z", d], 128 * w, ("f", i, 1 + d))] if alone else []),
                after=start,
            )

        def emit_z_last():
            if kind == "A":
                for d in range(2):
                    arrive(("z", i, d, 4), z_r.at[d, 2, 0])
                gh_out[:, mine] = a_sum[0, z] + z_r[0, 2, 0].astype(F32) + z_r[1, 2, 0].astype(F32)
                return
            z_sum = bufs[f"z_sum{i}"]
            for d in range(2):
                arrive(("z", i, d, 4), z_r.at[d, 2])
            z_sum[...] = z_part(0, 0, n) + z_r[0, 2].astype(F32) + z_r[1, 2].astype(F32)
            for u, device in enumerate((partner, cross, {"y": opposite})):
                f_s[u] = z_sum[device["y"]].astype(BF16)
                send(("f", i, u), f_s.at[u], f_r.at[u], device)

        def emit_last():
            for u in range(3):
                arrive(("f", i, u), f_r.at[u])
            got = [f_r[u].astype(F32) for u in range(3)]
            if kind == "A":
                gh_out[:, theirs] = got[0] + got[1] + got[2]
            elif paired:
                gh_out[:, mine] = bufs[f"z_sum{i}"][y] + got[1]
                gh_out[:, theirs] = got[0] + got[2]
            else:
                gh_out[:, mine] = bufs[f"z_sum{i}"][y] + got[0] + got[1] + got[2]

        for d in range(2):
            for step in range(1, 5):
                z_step(d, step)
        final = [] if kind == "A" else [
            (pair_link, 128 * w, ("f", i, 0)),
            (cross_link, 128 * w, ("f", i, 1)),
            (cross_link, 256 * w, ("f", i, 2)),
        ]
        op(
            ("zf", i),
            emit_z_last,
            0.012 if kind == "A" else cost(256),
            rank,
            recv=[("z", i, d, 4) for d in range(2)],
            send=final,
            after=start,
        )
        op(("ff", i), emit_last, 0.02, rank, recv=[("f", i, u) for u in range(3)], after=[("zf", i)])

    for i in range(len(TABLE)):
        chunk(i)

    hops = (2, 1, 3, 0)

    def back(slot, h):
        return lax.dot_general(
            grad[halves[h], :], head[slot], (((1,), (1,)), ((), ())), preferred_element_type=F32
        )

    def hs_step(n):
        def emit():
            slot = vocab_at(hops[n], 1)
            for h in range(2):
                bufs["hs_s"][n, halves[h], :] = back(slot, h).astype(BF16)
            send(("hs", n), bufs["hs_s"].at[n], bufs["hs_r"].at[n], to_sib)

        op(("hs", n), emit, 0.76, 30, send=[("c", 262144, ("hs", n))])

    def hg_step(n):
        def emit():
            arrive(("hs", n), bufs["hs_r"].at[n])
            if n == 1 or n == 2:
                d = n - 1
                arrive(("h1", d), bufs["h1_r"].at[d])
            if n == 3:
                for d in range(2):
                    arrive(("h2", d), bufs["h2_r"].at[d])
            slot = vocab_at(hops[n], 0)
            for h in range(2):
                rows = halves[h]
                value = back(slot, h) + bufs["hs_r"][n, rows, :].astype(F32)
                if n == 0:
                    bufs["h1_s"][h] = value.astype(BF16)
                    send(("h1", h), bufs["h1_s"].at[h], bufs["h1_r"].at[h], toward("x", h))
                elif n < 3:
                    if h == n - 1:
                        value = value + bufs["h1_r"][h].astype(F32)
                    bufs["h2_s"][n - 1, rows, :] = value.astype(BF16)
                else:
                    got = [bufs["h2_r"][d, rows, :].astype(F32) for d in range(2)]
                    hg_out[rows, :] = (value + got[0] + got[1]).astype(BF16)
            if n == 1 or n == 2:
                d = n - 1
                send(("h2", d), bufs["h2_s"].at[d], bufs["h2_r"].at[d], toward("x", d))

        recv = [("hs", n)] + {0: [], 1: [("h1", 0)], 2: [("h1", 1)], 3: [("h2", 0), ("h2", 1)]}[n]
        sends = {
            0: [("x+", 131072, ("h1", 0)), ("x-", 131072, ("h1", 1))],
            1: [("x+", 262144, ("h2", 0))],
            2: [("x-", 262144, ("h2", 1))],
            3: [],
        }[n]
        op(("hg", n), emit, 0.77 if n else 1.45, 30, recv=recv, send=sends)

    for n in range(4):
        hs_step(n)
        hg_step(n)

    def divergence():
        def emit():
            shared("x_cross")
            ref, peaks = bufs["x_cross"], bufs["x_tea"]
            peak, total = merged(peaks)
            s_peak, s_total = merged(bufs["x_stu"])
            cross = None
            for k in range(8):
                term = ref[k, 0:4, :] * jnp.exp(peaks[k, 0:4, :] - peak)
                cross = term if cross is None else cross + term
            kl_out[...] = cross / total - peak - jnp.log(total) + s_peak + jnp.log(s_total)

        op("kl", emit, 0.05, 40, after=[("hg", 3)])

    divergence()

    order, _ = in_order(ops)
    for step in order:
        step["emit"]()

    for copy in sent:
        copy.wait_send()


def handed_on(*refs):
    for src, dst in zip(refs[:3], refs[3:]):
        dst[...] = src[...]


def per_device(hidden_states, teacher_logits, head_weight):
    vmem = pl.BlockSpec(memory_space=pltpu.VMEM)
    hbm = pl.BlockSpec(memory_space=pl.ANY)
    kl, hidden_grad, head_grad = pl.pallas_call(
        kernel,
        out_shape=(
            jax.ShapeDtypeStruct((4, LANES), F32),
            jax.ShapeDtypeStruct((ROWS, PART), BF16),
            jax.ShapeDtypeStruct((64, VOCAB), F32),
        ),
        in_specs=[hbm, hbm, hbm],
        out_specs=(vmem, vmem, vmem),
        scratch_shapes=[pltpu.VMEM(*SCRATCH[k]) for k in NAMES]
        + [
            pltpu.SemaphoreType.DMA((10,)),
            pltpu.SemaphoreType.DMA((N_COPIES,)),
            pltpu.SemaphoreType.DMA((N_COPIES,)),
        ],
        compiler_params=pltpu.CompilerParams(
            collective_id=0, has_side_effects=True, vmem_limit_bytes=66_000_000
        ),
    )(hidden_states, teacher_logits, head_weight)
    kl, hidden_grad, head_grad = pl.pallas_call(
        handed_on,
        out_shape=tuple(jax.ShapeDtypeStruct(v.shape, v.dtype) for v in (kl, hidden_grad, head_grad)),
        in_specs=[vmem] * 3,
        out_specs=(vmem,) * 3,
    )(kl, hidden_grad, head_grad)
    return kl.reshape(ROWS), hidden_grad, head_grad


def solution(mesh):
    split = Mesh(mesh.devices.reshape(NY, NZ, NX, 2), ("y", "z", "x", "c"))
    dp, vocab = ("y", "z"), ("x", "c")
    return jax.shard_map(
        per_device,
        mesh=split,
        in_specs=(P(dp, vocab), P(dp, vocab), P(None, vocab)),
        out_specs=(P(dp), P(dp, vocab), P(dp, vocab)),
        check_vma=False,
    )
```

```python
import jax
import jax.numpy as jnp
from jax import lax
from jax.experimental import pallas as pl
from jax.experimental.pallas import tpu as pltpu
from jax.sharding import Mesh
from jax.sharding import PartitionSpec as P

MESH = pl.DeviceIdType.MESH
F32, BF16 = jnp.float32, jnp.bfloat16
NY, NZ, NX = 4, 8, 4
ROWS, WIDTH, VOCAB, PART = 512, 2048, 2048, 256
GRAD_SCALE = 8.0
LANES = 128

CHUNKS = tuple((k, 128) for k in "ZAabAbbbAa")
RANKS = (0.8, 6.2, 8.9, 2.0, 9.1, 6.0, 6.7, 2.5, 8.9, 6.5)
SWAPS = (1, 2, 9, 3, 7, 6, 5, 4, 0, 8)
FIRST = -3


def chunk_table():
    table, begin, half = [], 0, 0
    for (kind, width), rank, turn in zip(CHUNKS, RANKS, SWAPS):
        paired = kind not in "Bb"
        table.append(dict(kind=kind.upper(), m=int(kind.islower()), w=width, paired=paired, at=begin, half=half, rank=rank, turn=turn))
        begin += width * (2 if paired else 1)
        half += width if paired else 0
    assert begin == VOCAB
    return table, half


TABLE, HALF_WIDTH = chunk_table()
EARLY = {("m", 0, "O"): 2.0, ("m", 1, "LR0"): 3.3, ("m", 1, "LR1"): 6.1}


RATE = 46.0e3


def in_order(ops):
    done, arrived, link_free, now, order = {}, dict(EARLY), {"x+": 2.9, "x-": 2.9}, 0.0, []
    left = list(ops)
    while left:
        best = None
        for rank, op in enumerate(left):
            if any(d not in done for d in op["after"]) or any(r not in arrived for r in op["recv"]):
                continue
            ready = max([now] + [arrived[r] for r in op["recv"]])
            key = (ready, op["rank"], rank)
            if best is None or key < best[0]:
                best = (key, op)
        (ready, _, _), op = best
        now = ready + op["time"]
        done[op["name"]] = now
        for link, size, key in op["send"]:
            begin = max(now, link_free.get(link, 0.0))
            wire = size / (RATE if link != "c" else 600e3)
            link_free[link] = begin + wire
            hops = 0.75 if link[0] == "z" and key[0] == "f" or link[0] in "pq" and key[0] == "f" and key[2] == 2 else 0.0
            arrived[key] = begin + wire + (2.8 + hops if link != "c" else 1.0)
        order.append(op)
        left.remove(op)
    return order, now


def fold(op, tiles):
    tiles = list(tiles)
    while len(tiles) > 1:
        pairs = [op(a, b) for a, b in zip(tiles[::2], tiles[1::2])]
        tiles = pairs + ([tiles[-1]] if len(tiles) % 2 else [])
    return tiles[0]


def lane_tiles(value):
    return [value[:, i : i + LANES] for i in range(0, value.shape[1], LANES)]


SCRATCH = dict(
    hid=((8, ROWS, PART), BF16),
    hid_t=((3, NY, NZ, 64, ROWS), BF16),
    tea=((ROWS, VOCAB), BF16),
    head=((8, PART, VOCAB), BF16),
    stu=((ROWS, VOCAB), F32),
    stu_exp=((ROWS, VOCAB), F32),
    tea_exp=((ROWS, VOCAB), F32),
    grad=((ROWS, VOCAB), BF16),
    part_a=((ROWS, LANES), F32),
    part_b=((ROWS, LANES), F32),
    part_c=((ROWS, LANES), F32),
    tea_max=((ROWS, LANES), F32),
    x_tea=((8, 8, LANES), F32),
    x_stu=((8, 8, LANES), F32),
    x_cross=((8, 8, LANES), F32),
    hid_m=((2, 8, ROWS, PART), BF16),
    grad_m=((ROWS, HALF_WIDTH), BF16),
    hs_s=((4, ROWS, PART), BF16),
    hs_r=((4, ROWS, PART), BF16),
    h1_s=((2, 256, PART), BF16),
    h1_r=((2, 256, PART), BF16),
    h2_s=((2, ROWS, PART), BF16),
    h2_r=((2, ROWS, PART), BF16),
)
for _i, _c in enumerate(TABLE):
    _w, _n = _c["w"], 2 if _c["kind"] == "A" else 4
    for _side in "sr":
        SCRATCH[f"z1_{_side}{_i}"] = ((2, _n // 2, 64, _w), BF16)
        SCRATCH[f"z_{_side}{_i}"] = ((2, 3, _n, 64, _w), BF16)
        SCRATCH[f"f_{_side}{_i}"] = ((3, 64, _w), BF16)
        if _c["kind"] == "A":
            SCRATCH[f"x_{_side}{_i}"] = ((2, ROWS, _w), BF16)
    if _c["kind"] == "A":
        SCRATCH[f"a_sum{_i}"] = ((2, NZ, 64, _w), F32)
    else:
        SCRATCH[f"z_sum{_i}"] = ((4, 64, _w), F32)
NAMES = tuple(SCRATCH)
N_COPIES = 230
WIDE = 1024


def kernel(hidden_in, teacher_in, head_in, kl_out, hg_out, gh_out, *rest):
    bufs = dict(zip(NAMES, rest))
    load_sem, send_sem, recv_sem = rest[len(NAMES) :]
    hid, hid_t, tea, head, stu = (bufs[k] for k in ("hid", "hid_t", "tea", "head", "stu"))
    stu_exp, tea_exp, grad = bufs["stu_exp"], bufs["tea_exp"], bufs["grad"]
    part_a, part_b, tea_max = bufs["part_a"], bufs["part_b"], bufs["tea_max"]

    y, z, x, c = (lax.axis_index(a) for a in ("y", "z", "x", "c"))

    def near(axis, delta):
        here, size = {"y": (y, NY), "z": (z, NZ), "x": (x, NX)}[axis]
        return lax.rem(here + (delta % size), size)

    def vocab_at(dx, dc):
        return 2 * near("x", dx) + (c if dc == 0 else 1 - c)

    me, sib = vocab_at(0, 0), vocab_at(0, 1)
    to_sib = {"c": 1 - c}
    peers = [(dx, dc) for dx in range(NX) for dc in range(2) if (dx, dc) != (0, 0)]

    def peer(dx, dc):
        return {"x": near("x", dx), "c": c if dc == 0 else 1 - c}

    numbers, sent = {}, []

    def remote(key, src, dst, device):
        number = numbers.setdefault(key, len(numbers))
        assert number < N_COPIES
        return pltpu.make_async_remote_copy(
            src_ref=src,
            dst_ref=dst,
            send_sem=send_sem.at[number],
            recv_sem=recv_sem.at[number],
            device_id=device,
            device_id_type=MESH,
        )

    def send(key, src, dst, device):
        copy = remote(key, src, dst, device)
        copy.start()
        sent.append(copy)

    def arrive(key, dst, device=None):
        remote(key, dst, dst, to_sib).wait_recv()

    loads = [pltpu.make_async_copy(hidden_in, hid.at[me], load_sem.at[0])]
    loads[0].start()
    slots = [vocab_at(*p) for p in ((0, 0), (0, 1), (3, 0), (1, 0), (3, 1), (1, 1), (2, 0), (2, 1))]
    own, sibling, left, right, left_s, right_s, far, far_s = slots
    head_loads = []
    for k, slot in enumerate(slots):
        rows = pl.ds(pl.multiple_of(slot * PART, PART), PART)
        head_loads.append(pltpu.make_async_copy(head_in.at[rows], head.at[slot], load_sem.at[1 + k]))
    tea_load = pltpu.make_async_copy(teacher_in, tea, load_sem.at[9])
    head_loads[0].start()
    head_loads[1].start()
    tea_load.start()
    for copy in head_loads[2:]:
        copy.start()

    barrier = pltpu.get_barrier_semaphore()
    around = [peer(*p) for p in peers] + [{"y": near("y", d)} for d in (1, -1, 2)] + [{"z": near("z", d)} for d in (1, -1)]
    around += [{"y": near("y", d), "z": near("z", e)} for d in (1, -1) for e in (1, -1)]
    for device in around:
        pl.semaphore_signal(barrier, inc=1, device_id=device, device_id_type=MESH)
    pl.semaphore_wait(barrier, len(around))

    halves = (pl.ds(0, 256), pl.ds(256, 256))
    x_right, x_left = {"x": near("x", 1)}, {"x": near("x", -1)}
    loads[0].wait()

    def half(slot, h):
        return hid.at[slot, halves[h]]

    def give(key, slot, h, device):
        send(key, half(slot, h), half(slot, h), device)

    give("L0", own, 0, x_right)
    give("R1", own, 1, x_left)
    send("own", hid.at[own], hid.at[own], to_sib)
    give("L1", own, 1, x_right)
    give("R0", own, 0, x_left)
    hid_m = bufs["hid_m"]
    rem2 = lax.rem(y, 2)
    partners = ({"y": y + 1 - 2 * rem2}, {"y": 3 - y})
    for m in range(2):
        send(("m", m, "y"), hid.at[own], hid_m.at[m, own], partners[m])

    def half_m(m, slot, h):
        return hid_m.at[m, slot, halves[h]]

    def give_m(m, key, slot, h, device):
        send(("m", m, key), half_m(m, slot, h), half_m(m, slot, h), device)

    def arrive_m(m, key, slot, h):
        arrive(("m", m, key), half_m(m, slot, h))

    def first_m(m):
        arrive(("m", m, "y"), hid_m.at[m, own])
        give_m(m, "L0", own, 0, x_right)
        give_m(m, "R1", own, 1, x_left)
        send(("m", m, "own"), hid_m.at[m, own], hid_m.at[m, own], to_sib)
        give_m(m, "L1", own, 1, x_right)
        give_m(m, "R0", own, 0, x_left)

    def second_m(m):
        arrive_m(m, "L0", left, 0)
        give_m(m, "O0", left, 0, x_right)
        give_m(m, "SL0", left, 0, to_sib)
        arrive_m(m, "R1", right, 1)
        give_m(m, "O1", right, 1, x_left)
        give_m(m, "SR1", right, 1, to_sib)

    def third_m(m):
        arrive_m(m, "L1", left, 1)
        give_m(m, "SL1", left, 1, to_sib)
        arrive_m(m, "R0", right, 0)
        give_m(m, "SR0", right, 0, to_sib)

    def fourth_m(m):
        for h in range(2):
            arrive_m(m, f"O{h}", far, h)
            give_m(m, f"SO{h}", far, h, to_sib)

    def turn(which, source):
        @pl.loop(0, NY)
        def _(j):
            for u in range(2):
                for b in range(4):
                    rows = slice(b * LANES, (b + 1) * LANES)
                    turned = source(2 * j + u, rows).T
                    hid_t[which, j, 4 * u : 4 * u + 4, :, rows] = turned.reshape(4, 64, LANES)

    def fifth_m(m):
        arrive(("m", m, "own"), hid_m.at[m, sibling])
        for h in range(2):
            arrive_m(m, f"SL{h}", left_s, h)
            arrive_m(m, f"SR{h}", right_s, h)
            arrive_m(m, f"SO{h}", far_s, h)
        turn(1 + m, lambda slot, rows: hid_m[m, slot, rows, :])

    def logits(ks, first=False):
        for k in ks:
            head_loads[k].wait()

        @pl.loop(0, VOCAB // WIDE)
        def _(n):
            cols = pl.ds(pl.multiple_of(n * WIDE, WIDE), WIDE)
            value = sum(
                jnp.dot(hid[slots[k]], head[slots[k], :, cols], preferred_element_type=F32) for k in ks
            )
            if first:
                stu[:, cols] = value
            else:
                stu[:, cols] += value

    def row_blocks(size, body):
        @pl.loop(0, ROWS // size)
        def _(n):
            body(pl.ds(pl.multiple_of(n * size, size), size))

    def spread_max(ref_in, ref_out):
        ref_out[...] = jnp.broadcast_to(jnp.max(ref_in[...], axis=1, keepdims=True), (ROWS, LANES))

    def tea_peaks(rows):
        part_a[rows, :] = fold(jnp.maximum, lane_tiles(tea[rows, :].astype(F32)))

    def tea_terms(rows):
        peak = tea_max[rows, :]
        total = None
        for i in range(0, VOCAB, LANES):
            term = jnp.exp(tea[rows, i : i + LANES].astype(F32) - peak)
            tea_exp[rows, i : i + LANES] = term
            total = term if total is None else total + term
        part_b[rows, :] = total

    def compact(ref, slot, at, peaks_ref, sums_ref=part_b):
        for b in range(4):
            rows = slice(b * LANES, (b + 1) * LANES)
            if peaks_ref is not None:
                ref[slot, b : b + 1, :] = peaks_ref[rows, :].T[0:1, :]
            ref[slot, at + b : at + b + 1, :] = jnp.sum(sums_ref[rows, :].T, axis=0, keepdims=True)

    def share(name):
        ref = bufs[name]
        for dx, dc in peers:
            send((name, dx, dc), ref.at[me], ref.at[me], peer(dx, dc))

    def shared(name):
        ref = bufs[name]
        for dx, dc in peers:
            slot = vocab_at(-dx, dc)
            arrive((name, dx, dc), ref.at[slot])

    def merged(ref):
        peak = fold(jnp.maximum, [ref[k, 0:4, :] for k in range(8)])
        total = None
        for k in range(8):
            term = ref[k, 4:8, :] * jnp.exp(ref[k, 0:4, :] - peak)
            total = term if total is None else total + term
        return peak, total

    def spread(value, ref):
        for b in range(4):
            ref[b * LANES : (b + 1) * LANES, :] = jnp.broadcast_to(
                value[b : b + 1, :], (LANES, LANES)
            ).T

    arrive("own", hid.at[sibling])
    logits((0, 1), first=True)
    tea_load.wait()
    row_blocks(32, tea_peaks)
    spread_max(part_a, tea_max)
    arrive("L0", half(left, 0))
    give("O0", left, 0, x_right)
    give("SL0", left, 0, to_sib)
    arrive("R1", half(right, 1))
    give("O1", right, 1, x_left)
    give("SR1", right, 1, to_sib)
    row_blocks(16, tea_terms)
    arrive("L1", half(left, 1))
    give("SL1", left, 1, to_sib)
    arrive("R0", half(right, 0))
    give("SR0", right, 0, to_sib)
    compact(bufs["x_tea"], me, 4, tea_max)
    share("x_tea")
    first_m(0)
    logits((2, 3))
    arrive("SL0", half(left_s, 0))
    arrive("SL1", half(left_s, 1))
    arrive("SR0", half(right_s, 0))
    arrive("SR1", half(right_s, 1))
    logits((4, 5))
    arrive("O0", half(far, 0))
    give("SO0", far, 0, to_sib)
    arrive("O1", half(far, 1))
    give("SO1", far, 1, to_sib)
    logits((6,))
    arrive("SO0", half(far_s, 0))
    arrive("SO1", half(far_s, 1))
    logits((7,))

    def stu_peaks(rows):
        part_a[rows, :] = fold(jnp.maximum, lane_tiles(stu[rows, :]))

    def stu_terms(rows):
        peak = part_a[rows, :]
        total = None
        for i in range(0, VOCAB, LANES):
            term = jnp.exp(stu[rows, i : i + LANES] - peak)
            stu_exp[rows, i : i + LANES] = term
            total = term if total is None else total + term
        part_b[rows, :] = total

    def cross_terms(rows):
        total = None
        for i in range(0, VOCAB, LANES):
            cols = slice(i, i + LANES)
            term = tea_exp[rows, cols] * (tea[rows, cols].astype(F32) - stu[rows, cols])
            total = term if total is None else total + term
        bufs["part_c"][rows, :] = total

    row_blocks(32, stu_peaks)
    spread_max(part_a, part_a)
    row_blocks(16, stu_terms)
    compact(bufs["x_stu"], me, 4, part_a)
    share("x_stu")

    turn(0, lambda slot, rows: hid[slot, rows, :])

    shared("x_tea")
    tea_peak, tea_total = merged(bufs["x_tea"])
    spread(GRAD_SCALE * jnp.exp(bufs["x_tea"][me, 0:4, :] - tea_peak) / tea_total, part_b)
    second_m(0)
    third_m(0)
    first_m(1)
    row_blocks(16, cross_terms)
    bufs["x_cross"][me, 4:8, :] = jnp.zeros((4, LANES), F32)
    compact(bufs["x_cross"], me, 0, None, bufs["part_c"])
    share("x_cross")
    shared("x_stu")
    stu_peak, stu_total = merged(bufs["x_stu"])
    spread(GRAD_SCALE * jnp.exp(bufs["x_stu"][me, 0:4, :] - stu_peak) / stu_total, part_a)

    def grads(rows):
        stu_scale, tea_scale = part_a[rows, :], part_b[rows, :]
        for i in range(0, VOCAB, LANES):
            cols = slice(i, i + LANES)
            grad[rows, cols] = (stu_exp[rows, cols] * stu_scale - tea_exp[rows, cols] * tea_scale).astype(BF16)

    row_blocks(16, grads)

    ops = []

    def op(name, emit, time, rank, recv=(), send=(), after=()):
        ops.append(
            dict(name=name, emit=emit, time=time, rank=rank, recv=list(recv), send=list(send), after=list(after))
        )

    links = {("y", 0): "y+", ("y", 1): "y-", ("z", 0): "z+", ("z", 1): "z-", ("x", 0): "x+", ("x", 1): "x-"}

    def toward(axis, d):
        return {axis: near(axis, 1 if d == 0 else -1)}

    def signed(d, n):
        return n if d == 0 else -n

    grad_m = bufs["grad_m"]
    high = (y * (3 - y), y - rem2)

    op("g0o", lambda: fourth_m(0), 0.01, -5, recv=[("m", 0, "O")], send=[("c", 262144, ("m", 0, "SO"))])
    op("g0t", lambda: fifth_m(0), 0.78, -5, recv=[("m", 0, "SO")])
    op(
        "g1a",
        lambda: second_m(1),
        0.01,
        -3,
        recv=[("m", 1, "LR0")],
        send=[("x+", 131072, ("m", 1, "O0")), ("x-", 131072, ("m", 1, "O1")), ("c", 262144, ("m", 1, "S0"))],
    )
    op("g1b", lambda: third_m(1), 0.01, -3, recv=[("m", 1, "LR1")], send=[("c", 262144, ("m", 1, "S1"))], after=["g1a"])
    op(
        "g1o",
        lambda: fourth_m(1),
        0.01,
        -3,
        recv=[("m", 1, "O0"), ("m", 1, "O1")],
        send=[("c", 262144, ("m", 1, "SO"))],
        after=["g1b"],
    )
    op("g1t", lambda: fifth_m(1), 0.78, -5, recv=[("m", 1, k) for k in ("SO", "S0", "S1")])

    def chunk(i):
        info = TABLE[i]
        kind, m, w, paired, at, half_at = (info[k] for k in ("kind", "m", "w", "paired", "at", "half"))
        rank = info["rank"]
        pair_link, cross_link = ("p", "q") if m == 0 else ("q", "p")
        partner, cross = partners[m], partners[1 - m]
        opposite = lax.rem(y + 2, NY)
        mine = pl.ds(pl.multiple_of(at + high[m] * (w // 2), LANES), w) if paired else pl.ds(at, w)
        theirs = pl.ds(pl.multiple_of(at + (2 - high[m]) * (w // 2), LANES), w) if paired else None
        got_cols = pl.ds(half_at, w)
        n = 2 if kind == "A" else 4
        z1_s, z1_r, z_s, z_r = (bufs[f"{k}{i}"] for k in ("z1_s", "z1_r", "z_s", "z_r"))
        f_s, f_r = (bufs[f"{k}{i}"] for k in ("f_s", "f_r"))

        def formed(rows_of):
            value = jnp.dot(rows_of(0), grad[:, mine], preferred_element_type=F32)
            if paired:
                value = value + jnp.dot(rows_of(1 + m), grad_m[:, got_cols], preferred_element_type=F32)
            return value

        def cost(rows):
            if kind == "A":
                return 0.71 if w == 128 else 1.1
            return ((0.3 if paired else 0.24) if rows == 256 else (0.22 if paired else 0.19)) * (1 if w == 128 else 1.5)

        start = []
        if paired:

            def emit_swap():
                send(("p", i), grad.at[:, theirs], grad_m.at[:, got_cols], partner)

            def emit_swapped():
                arrive(("p", i), grad_m.at[:, got_cols])

            op(("p", i), emit_swap, 0.02, -10 + 0.01 * info["turn"], send=[(pair_link, 1024 * w, ("p", i))])
            op(("pr", i), emit_swapped, 0.01, rank, recv=[("p", i)], after=[f"g{m}t"])
            start = [("pr", i)]

        if kind == "A":
            a_sum, x_s, x_r = (bufs[f"{k}{i}"] for k in ("a_sum", "x_s", "x_r"))

            def emit_cross():
                for u, j in enumerate((cross["y"], opposite)):
                    x_s[u] = formed(lambda t: hid_t[t, j].reshape(ROWS, ROWS)).astype(BF16)
                send(("q", i), x_s, x_r, cross)

            def emit_kept():
                arrive(("q", i), x_r)
                for u, j in enumerate((y, partner["y"])):
                    value = formed(lambda t: hid_t[t, j].reshape(ROWS, ROWS)) + x_r[u].astype(F32)
                    a_sum[u] = value.reshape(NZ, 64, w)
                f_s[0] = a_sum[1, z].astype(BF16)
                send(("f", i, 0), f_s.at[0], f_r.at[0], partner)

            op(("q", i), emit_cross, cost(1024), rank, send=[(cross_link, 2048 * w, ("q", i))], after=start)
            op(
                ("qf", i),
                emit_kept,
                cost(1024),
                rank,
                recv=[("q", i)],
                send=[(pair_link, 128 * w, ("f", i, 0))],
                after=start,
            )
            start = [("qf", i)]

        def z_part(k, lo, count):
            if kind == "A":
                return a_sum[lo : lo + count, near("z", k)]
            value = formed(lambda t: hid_t[t, lo : lo + count, near("z", k)].reshape(64 * count, ROWS))
            return value.reshape(count, 64, w)

        h = n // 2

        def z_step(d, step):
            dest = signed(d, 5 - step)
            lo = d * h
            src, dst = (z1_s.at[d], z1_r.at[d]) if step == 1 else (z_s.at[d, step - 2], z_r.at[d, step - 2])

            def emit():
                if step == 1:
                    z1_s[d] = z_part(dest, lo, h).astype(BF16)
                elif step == 2:
                    arrive(("z", i, d, 1), z1_r.at[d])
                    z_s[d, 0, h - lo : n - lo] = z_part(dest, h - lo, h).astype(BF16)
                    z_s[d, 0, lo : lo + h] = (z_part(dest, lo, h) + z1_r[d].astype(F32)).astype(BF16)
                else:
                    arrive(("z", i, d, step - 1), z_r.at[d, step - 3])
                    z_s[d, step - 2] = (z_part(dest, 0, n) + z_r[d, step - 3].astype(F32)).astype(BF16)
                if kind == "A" and step == 4:
                    send(("z", i, d, 4), src.at[0], dst.at[0], toward("z", d))
                    send(("f", i, 1 + d), src.at[1], f_r.at[1 + d], {**partner, **toward("z", d)})
                else:
                    send(("z", i, d, step), src, dst, toward("z", d))

            time = 0.012 if kind == "A" else cost(128 if step == 1 else 256)
            alone = kind == "A" and step == 4
            op(
                ("z", i, d, step),
                emit,
                time,
                rank + (FIRST if step == 1 else 0),
                recv=[("z", i, d, step - 1)] if step > 1 else [],
                send=[(links["z", d], 128 * w * (1 if alone else h if step == 1 else n), ("z", i, d, step))]
                + ([(links["z", d], 128 * w, ("f", i, 1 + d))] if alone else []),
                after=start,
            )

        def emit_z_last():
            if kind == "A":
                for d in range(2):
                    arrive(("z", i, d, 4), z_r.at[d, 2, 0])
                gh_out[:, mine] = a_sum[0, z] + z_r[0, 2, 0].astype(F32) + z_r[1, 2, 0].astype(F32)
                return
            z_sum = bufs[f"z_sum{i}"]
            for d in range(2):
                arrive(("z", i, d, 4), z_r.at[d, 2])
            z_sum[...] = z_part(0, 0, n) + z_r[0, 2].astype(F32) + z_r[1, 2].astype(F32)
            for u, device in enumerate((partner, cross, {"y": opposite})):
                f_s[u] = z_sum[device["y"]].astype(BF16)
                send(("f", i, u), f_s.at[u], f_r.at[u], device)

        def emit_last():
            for u in range(3):
                arrive(("f", i, u), f_r.at[u])
            got = [f_r[u].astype(F32) for u in range(3)]
            if kind == "A":
                gh_out[:, theirs] = got[0] + got[1] + got[2]
            elif paired:
                gh_out[:, mine] = bufs[f"z_sum{i}"][y] + got[1]
                gh_out[:, theirs] = got[0] + got[2]
            else:
                gh_out[:, mine] = bufs[f"z_sum{i}"][y] + got[0] + got[1] + got[2]

        for d in range(2):
            for step in range(1, 5):
                z_step(d, step)
        final = [] if kind == "A" else [
            (pair_link, 128 * w, ("f", i, 0)),
            (cross_link, 128 * w, ("f", i, 1)),
            (cross_link, 256 * w, ("f", i, 2)),
        ]
        op(
            ("zf", i),
            emit_z_last,
            0.012 if kind == "A" else cost(256),
            rank,
            recv=[("z", i, d, 4) for d in range(2)],
            send=final,
            after=start,
        )
        op(("ff", i), emit_last, 0.02, rank, recv=[("f", i, u) for u in range(3)], after=[("zf", i)])

    for i in range(len(TABLE)):
        chunk(i)

    hops = (2, 1, 3, 0)

    def back(slot, h):
        return lax.dot_general(
            grad[halves[h], :], head[slot], (((1,), (1,)), ((), ())), preferred_element_type=F32
        )

    def hs_step(n):
        def emit():
            slot = vocab_at(hops[n], 1)
            for h in range(2):
                bufs["hs_s"][n, halves[h], :] = back(slot, h).astype(BF16)
            send(("hs", n), bufs["hs_s"].at[n], bufs["hs_r"].at[n], to_sib)

        op(("hs", n), emit, 0.76, 30, send=[("c", 262144, ("hs", n))])

    def hg_step(n):
        def emit():
            arrive(("hs", n), bufs["hs_r"].at[n])
            if n == 1 or n == 2:
                d = n - 1
                arrive(("h1", d), bufs["h1_r"].at[d])
            if n == 3:
                for d in range(2):
                    arrive(("h2", d), bufs["h2_r"].at[d])
            slot = vocab_at(hops[n], 0)
            for h in range(2):
                rows = halves[h]
                value = back(slot, h) + bufs["hs_r"][n, rows, :].astype(F32)
                if n == 0:
                    bufs["h1_s"][h] = value.astype(BF16)
                    send(("h1", h), bufs["h1_s"].at[h], bufs["h1_r"].at[h], toward("x", h))
                elif n < 3:
                    if h == n - 1:
                        value = value + bufs["h1_r"][h].astype(F32)
                    bufs["h2_s"][n - 1, rows, :] = value.astype(BF16)
                else:
                    got = [bufs["h2_r"][d, rows, :].astype(F32) for d in range(2)]
                    hg_out[rows, :] = (value + got[0] + got[1]).astype(BF16)
            if n == 1 or n == 2:
                d = n - 1
                send(("h2", d), bufs["h2_s"].at[d], bufs["h2_r"].at[d], toward("x", d))

        recv = [("hs", n)] + {0: [], 1: [("h1", 0)], 2: [("h1", 1)], 3: [("h2", 0), ("h2", 1)]}[n]
        sends = {
            0: [("x+", 131072, ("h1", 0)), ("x-", 131072, ("h1", 1))],
            1: [("x+", 262144, ("h2", 0))],
            2: [("x-", 262144, ("h2", 1))],
            3: [],
        }[n]
        op(("hg", n), emit, 0.77 if n else 1.45, 30, recv=recv, send=sends)

    for n in range(4):
        hs_step(n)
        hg_step(n)

    def divergence():
        def emit():
            shared("x_cross")
            ref, peaks = bufs["x_cross"], bufs["x_tea"]
            peak, total = merged(peaks)
            s_peak, s_total = merged(bufs["x_stu"])
            cross = None
            for k in range(8):
                term = ref[k, 0:4, :] * jnp.exp(peaks[k, 0:4, :] - peak)
                cross = term if cross is None else cross + term
            kl_out[...] = cross / total - peak - jnp.log(total) + s_peak + jnp.log(s_total)

        op("kl", emit, 0.05, 40, after=[("hg", 3)])

    divergence()

    order, _ = in_order(ops)
    for step in order:
        step["emit"]()

    for copy in sent:
        copy.wait_send()


def per_device(hidden_states, teacher_logits, head_weight):
    vmem = pl.BlockSpec(memory_space=pltpu.VMEM)
    hbm = pl.BlockSpec(memory_space=pl.ANY)
    kl, hidden_grad, head_grad = pl.pallas_call(
        kernel,
        out_shape=(
            pltpu.VMEM((4, LANES), F32),
            pltpu.VMEM((ROWS, PART), BF16),
            pltpu.VMEM((64, VOCAB), F32),
        ),
        in_specs=[hbm, hbm, hbm],
        out_specs=(vmem, vmem, vmem),
        scratch_shapes=[pltpu.VMEM(*SCRATCH[k]) for k in NAMES]
        + [
            pltpu.SemaphoreType.DMA((10,)),
            pltpu.SemaphoreType.DMA((N_COPIES,)),
            pltpu.SemaphoreType.DMA((N_COPIES,)),
        ],
        compiler_params=pltpu.CompilerParams(
            collective_id=0, has_side_effects=True, vmem_limit_bytes=64_500_000
        ),
    )(hidden_states, teacher_logits, head_weight)
    return kl.reshape(ROWS), hidden_grad, head_grad


def solution(mesh):
    split = Mesh(mesh.devices.reshape(NY, NZ, NX, 2), ("y", "z", "x", "c"))
    dp, vocab = ("y", "z"), ("x", "c")
    return jax.shard_map(
        per_device,
        mesh=split,
        in_specs=(P(dp, vocab), P(dp, vocab), P(None, vocab)),
        out_specs=(P(dp), P(dp, vocab), P(dp, vocab)),
        check_vma=False,
    )
```

```python
import jax
import jax.numpy as jnp
from jax import lax
from jax.experimental import pallas as pl
from jax.experimental.pallas import tpu as pltpu
from jax.sharding import Mesh
from jax.sharding import PartitionSpec as P

MESH = pl.DeviceIdType.MESH
F32, BF16 = jnp.float32, jnp.bfloat16
NY, NZ, NX = 4, 8, 4
ROWS, WIDTH, VOCAB, PART = 512, 2048, 2048, 256
GRAD_SCALE = 8.0
LANES = 128

CHUNKS = tuple((k, 128) for k in "ZAabAbbbAa")
RANKS = (0.8, 6.2, 8.9, 2.0, 9.1, 6.0, 6.7, 2.5, 8.9, 6.5)
SWAPS = (1, 2, 9, 3, 7, 6, 5, 4, 0, 8)
FIRST = -3
SWAP_FIRST = (0, 1, 8, 9)


def chunk_table():
    table, begin, half = [], 0, 0
    for (kind, width), rank, turn in zip(CHUNKS, RANKS, SWAPS):
        paired = kind not in "Bb"
        table.append(dict(kind=kind.upper(), m=int(kind.islower()), w=width, paired=paired, at=begin, half=half, rank=rank, turn=turn))
        begin += width * (2 if paired else 1)
        half += width if paired else 0
    assert begin == VOCAB
    return table, half


TABLE, HALF_WIDTH = chunk_table()
EARLY = {("m", 0, "O"): 2.0, ("m", 1, "LR0"): 3.3, ("m", 1, "LR1"): 6.1}


RATE = 46.0e3


def in_order(ops):
    done, arrived, link_free, now, order = {}, dict(EARLY), {"x+": 2.9, "x-": 2.9}, 0.0, []
    left = list(ops)
    while left:
        best = None
        for rank, op in enumerate(left):
            if any(d not in done for d in op["after"]) or any(r not in arrived for r in op["recv"]):
                continue
            ready = max([now] + [arrived[r] for r in op["recv"]])
            key = (ready, op["rank"], rank)
            if best is None or key < best[0]:
                best = (key, op)
        (ready, _, _), op = best
        now = ready + op["time"]
        done[op["name"]] = now
        for link, size, key in op["send"]:
            begin = max(now, link_free.get(link, 0.0))
            wire = size / (RATE if link != "c" else 600e3)
            link_free[link] = begin + wire
            hops = 0.75 if link[0] == "z" and key[0] == "f" or link[0] in "pq" and key[0] == "f" and key[2] == 2 else 0.0
            arrived[key] = begin + wire + (2.8 + hops if link != "c" else 1.0)
        order.append(op)
        left.remove(op)
    return order, now


def fold(op, tiles):
    tiles = list(tiles)
    while len(tiles) > 1:
        pairs = [op(a, b) for a, b in zip(tiles[::2], tiles[1::2])]
        tiles = pairs + ([tiles[-1]] if len(tiles) % 2 else [])
    return tiles[0]


def lane_tiles(value):
    return [value[:, i : i + LANES] for i in range(0, value.shape[1], LANES)]


SCRATCH = dict(
    hid=((8, ROWS, PART), BF16),
    hid_t=((3, NY, NZ, 64, ROWS), BF16),
    tea=((ROWS, VOCAB), BF16),
    head=((8, PART, VOCAB), BF16),
    stu=((ROWS, VOCAB), F32),
    stu_exp=((ROWS, VOCAB), F32),
    tea_exp=((ROWS, VOCAB), F32),
    grad=((ROWS, VOCAB), BF16),
    part_a=((ROWS, LANES), F32),
    part_b=((ROWS, LANES), F32),
    part_c=((ROWS, LANES), F32),
    tea_max=((ROWS, LANES), F32),
    x_tea=((8, 8, LANES), F32),
    x_stu=((8, 8, LANES), F32),
    x_cross=((8, 8, LANES), F32),
    hid_m=((2, 8, ROWS, PART), BF16),
    grad_m=((ROWS, HALF_WIDTH), BF16),
    hs_s=((4, ROWS, PART), BF16),
    hs_r=((4, ROWS, PART), BF16),
    h1_s=((2, 256, PART), BF16),
    h1_r=((2, 256, PART), BF16),
    h2_s=((2, ROWS, PART), BF16),
    h2_r=((2, ROWS, PART), BF16),
)
for _i, _c in enumerate(TABLE):
    _w, _n = _c["w"], 2 if _c["kind"] == "A" else 4
    for _side in "sr":
        SCRATCH[f"z1_{_side}{_i}"] = ((2, _n // 2, 64, _w), BF16)
        SCRATCH[f"z_{_side}{_i}"] = ((2, 3, _n, 64, _w), BF16)
        SCRATCH[f"f_{_side}{_i}"] = ((3, 64, _w), BF16)
        if _c["kind"] == "A":
            SCRATCH[f"x_{_side}{_i}"] = ((2, ROWS, _w), BF16)
    if _c["kind"] == "A":
        SCRATCH[f"a_sum{_i}"] = ((2, NZ, 64, _w), F32)
    else:
        SCRATCH[f"z_sum{_i}"] = ((4, 64, _w), F32)
NAMES = tuple(SCRATCH)
N_COPIES = 230
WIDE = 2048


def kernel(hidden_in, teacher_in, head_in, kl_out, hg_out, gh_out, *rest):
    bufs = dict(zip(NAMES, rest))
    load_sem, send_sem, recv_sem = rest[len(NAMES) :]
    hid, hid_t, tea, head, stu = (bufs[k] for k in ("hid", "hid_t", "tea", "head", "stu"))
    stu_exp, tea_exp, grad = bufs["stu_exp"], bufs["tea_exp"], bufs["grad"]
    part_a, part_b, tea_max = bufs["part_a"], bufs["part_b"], bufs["tea_max"]

    y, z, x, c = (lax.axis_index(a) for a in ("y", "z", "x", "c"))

    def near(axis, delta):
        here, size = {"y": (y, NY), "z": (z, NZ), "x": (x, NX)}[axis]
        return lax.rem(here + (delta % size), size)

    def vocab_at(dx, dc):
        return 2 * near("x", dx) + (c if dc == 0 else 1 - c)

    me, sib = vocab_at(0, 0), vocab_at(0, 1)
    to_sib = {"c": 1 - c}
    peers = [(dx, dc) for dx in range(NX) for dc in range(2) if (dx, dc) != (0, 0)]

    def peer(dx, dc):
        return {"x": near("x", dx), "c": c if dc == 0 else 1 - c}

    numbers, sent = {}, []

    def remote(key, src, dst, device):
        number = numbers.setdefault(key, len(numbers))
        assert number < N_COPIES
        return pltpu.make_async_remote_copy(
            src_ref=src,
            dst_ref=dst,
            send_sem=send_sem.at[number],
            recv_sem=recv_sem.at[number],
            device_id=device,
            device_id_type=MESH,
        )

    def send(key, src, dst, device):
        copy = remote(key, src, dst, device)
        copy.start()
        sent.append(copy)

    def arrive(key, dst, device=None):
        remote(key, dst, dst, to_sib).wait_recv()

    loads = [pltpu.make_async_copy(hidden_in, hid.at[me], load_sem.at[0])]
    loads[0].start()
    slots = [vocab_at(*p) for p in ((0, 0), (0, 1), (3, 0), (1, 0), (3, 1), (1, 1), (2, 0), (2, 1))]
    own, sibling, left, right, left_s, right_s, far, far_s = slots
    head_loads = []
    for k, slot in enumerate(slots):
        rows = pl.ds(pl.multiple_of(slot * PART, PART), PART)
        head_loads.append(pltpu.make_async_copy(head_in.at[rows], head.at[slot], load_sem.at[1 + k]))
    tea_load = pltpu.make_async_copy(teacher_in, tea, load_sem.at[9])
    head_loads[0].start()
    head_loads[1].start()
    tea_load.start()
    for copy in head_loads[2:]:
        copy.start()

    barrier = pltpu.get_barrier_semaphore()
    around = [peer(*p) for p in peers] + [{"y": near("y", d)} for d in (1, -1, 2)] + [{"z": near("z", d)} for d in (1, -1)]
    around += [{"y": near("y", d), "z": near("z", e)} for d in (1, -1) for e in (1, -1)]
    for device in around:
        pl.semaphore_signal(barrier, inc=1, device_id=device, device_id_type=MESH)
    pl.semaphore_wait(barrier, len(around))

    halves = (pl.ds(0, 256), pl.ds(256, 256))
    x_right, x_left = {"x": near("x", 1)}, {"x": near("x", -1)}
    loads[0].wait()

    def half(slot, h):
        return hid.at[slot, halves[h]]

    def give(key, slot, h, device):
        send(key, half(slot, h), half(slot, h), device)

    give("L0", own, 0, x_right)
    give("R1", own, 1, x_left)
    send("own", hid.at[own], hid.at[own], to_sib)
    give("L1", own, 1, x_right)
    give("R0", own, 0, x_left)
    hid_m = bufs["hid_m"]
    rem2 = lax.rem(y, 2)
    partners = ({"y": y + 1 - 2 * rem2}, {"y": 3 - y})
    for m in range(2):
        send(("m", m, "y"), hid.at[own], hid_m.at[m, own], partners[m])

    def half_m(m, slot, h):
        return hid_m.at[m, slot, halves[h]]

    def give_m(m, key, slot, h, device):
        send(("m", m, key), half_m(m, slot, h), half_m(m, slot, h), device)

    def arrive_m(m, key, slot, h):
        arrive(("m", m, key), half_m(m, slot, h))

    def first_m(m):
        arrive(("m", m, "y"), hid_m.at[m, own])
        give_m(m, "L0", own, 0, x_right)
        give_m(m, "R1", own, 1, x_left)
        send(("m", m, "own"), hid_m.at[m, own], hid_m.at[m, own], to_sib)
        give_m(m, "L1", own, 1, x_right)
        give_m(m, "R0", own, 0, x_left)

    def second_m(m):
        arrive_m(m, "L0", left, 0)
        give_m(m, "O0", left, 0, x_right)
        give_m(m, "SL0", left, 0, to_sib)
        arrive_m(m, "R1", right, 1)
        give_m(m, "O1", right, 1, x_left)
        give_m(m, "SR1", right, 1, to_sib)

    def third_m(m):
        arrive_m(m, "L1", left, 1)
        give_m(m, "SL1", left, 1, to_sib)
        arrive_m(m, "R0", right, 0)
        give_m(m, "SR0", right, 0, to_sib)

    def fourth_m(m):
        for h in range(2):
            arrive_m(m, f"O{h}", far, h)
            give_m(m, f"SO{h}", far, h, to_sib)

    def turn(which, source):
        @pl.loop(0, NY)
        def _(j):
            for u in range(2):
                for b in range(4):
                    rows = slice(b * LANES, (b + 1) * LANES)
                    turned = source(2 * j + u, rows).T
                    hid_t[which, j, 4 * u : 4 * u + 4, :, rows] = turned.reshape(4, 64, LANES)

    def fifth_m(m):
        arrive(("m", m, "own"), hid_m.at[m, sibling])
        for h in range(2):
            arrive_m(m, f"SL{h}", left_s, h)
            arrive_m(m, f"SR{h}", right_s, h)
            arrive_m(m, f"SO{h}", far_s, h)
        turn(1 + m, lambda slot, rows: hid_m[m, slot, rows, :])

    def logits(ks, first=False):
        for k in ks:
            head_loads[k].wait()

        @pl.loop(0, VOCAB // WIDE)
        def _(n):
            cols = pl.ds(pl.multiple_of(n * WIDE, WIDE), WIDE)
            value = sum(
                jnp.dot(hid[slots[k]], head[slots[k], :, cols], preferred_element_type=F32) for k in ks
            )
            if first:
                stu[:, cols] = value
            else:
                stu[:, cols] += value

    def row_blocks(size, body):
        @pl.loop(0, ROWS // size)
        def _(n):
            body(pl.ds(pl.multiple_of(n * size, size), size))

    def spread_max(ref_in, ref_out):
        ref_out[...] = jnp.broadcast_to(jnp.max(ref_in[...], axis=1, keepdims=True), (ROWS, LANES))

    def tea_peaks(rows):
        part_a[rows, :] = fold(jnp.maximum, lane_tiles(tea[rows, :].astype(F32)))

    def tea_terms(rows):
        peak = tea_max[rows, :]
        total = None
        for i in range(0, VOCAB, LANES):
            term = jnp.exp(tea[rows, i : i + LANES].astype(F32) - peak)
            tea_exp[rows, i : i + LANES] = term
            total = term if total is None else total + term
        part_b[rows, :] = total

    def compact(ref, slot, at, peaks_ref, sums_ref=part_b):
        for b in range(4):
            rows = slice(b * LANES, (b + 1) * LANES)
            if peaks_ref is not None:
                ref[slot, b : b + 1, :] = peaks_ref[rows, :].T[0:1, :]
            ref[slot, at + b : at + b + 1, :] = jnp.sum(sums_ref[rows, :].T, axis=0, keepdims=True)

    def share(name):
        ref = bufs[name]
        for dx, dc in peers:
            send((name, dx, dc), ref.at[me], ref.at[me], peer(dx, dc))

    def shared(name):
        ref = bufs[name]
        for dx, dc in peers:
            slot = vocab_at(-dx, dc)
            arrive((name, dx, dc), ref.at[slot])

    def merged(ref):
        peak = fold(jnp.maximum, [ref[k, 0:4, :] for k in range(8)])
        total = None
        for k in range(8):
            term = ref[k, 4:8, :] * jnp.exp(ref[k, 0:4, :] - peak)
            total = term if total is None else total + term
        return peak, total

    def spread(value, ref):
        for b in range(4):
            ref[b * LANES : (b + 1) * LANES, :] = jnp.broadcast_to(
                value[b : b + 1, :], (LANES, LANES)
            ).T

    arrive("own", hid.at[sibling])
    logits((0, 1), first=True)
    tea_load.wait()
    row_blocks(32, tea_peaks)
    spread_max(part_a, tea_max)
    arrive("L0", half(left, 0))
    give("O0", left, 0, x_right)
    give("SL0", left, 0, to_sib)
    arrive("R1", half(right, 1))
    give("O1", right, 1, x_left)
    give("SR1", right, 1, to_sib)
    row_blocks(16, tea_terms)
    arrive("L1", half(left, 1))
    give("SL1", left, 1, to_sib)
    arrive("R0", half(right, 0))
    give("SR0", right, 0, to_sib)
    compact(bufs["x_tea"], me, 4, tea_max)
    share("x_tea")
    first_m(0)
    logits((2, 3))
    arrive("SL0", half(left_s, 0))
    arrive("SL1", half(left_s, 1))
    arrive("SR0", half(right_s, 0))
    arrive("SR1", half(right_s, 1))
    logits((4, 5))
    arrive("O0", half(far, 0))
    give("SO0", far, 0, to_sib)
    arrive("O1", half(far, 1))
    give("SO1", far, 1, to_sib)
    logits((6,))
    arrive("SO0", half(far_s, 0))
    arrive("SO1", half(far_s, 1))
    logits((7,))

    def stu_peaks(rows):
        part_a[rows, :] = fold(jnp.maximum, lane_tiles(stu[rows, :]))

    def stu_terms(rows):
        peak = part_a[rows, :]
        total = None
        for i in range(0, VOCAB, LANES):
            term = jnp.exp(stu[rows, i : i + LANES] - peak)
            stu_exp[rows, i : i + LANES] = term
            total = term if total is None else total + term
        part_b[rows, :] = total

    def cross_terms(rows):
        total = None
        for i in range(0, VOCAB, LANES):
            cols = slice(i, i + LANES)
            term = tea_exp[rows, cols] * (tea[rows, cols].astype(F32) - stu[rows, cols])
            total = term if total is None else total + term
        bufs["part_c"][rows, :] = total

    row_blocks(32, stu_peaks)
    spread_max(part_a, part_a)
    row_blocks(16, stu_terms)
    compact(bufs["x_stu"], me, 4, part_a)
    share("x_stu")

    turn(0, lambda slot, rows: hid[slot, rows, :])

    shared("x_tea")
    tea_peak, tea_total = merged(bufs["x_tea"])
    spread(GRAD_SCALE * jnp.exp(bufs["x_tea"][me, 0:4, :] - tea_peak) / tea_total, part_b)
    second_m(0)
    third_m(0)
    first_m(1)
    row_blocks(16, cross_terms)
    bufs["x_cross"][me, 4:8, :] = jnp.zeros((4, LANES), F32)
    compact(bufs["x_cross"], me, 0, None, bufs["part_c"])
    share("x_cross")
    shared("x_stu")
    stu_peak, stu_total = merged(bufs["x_stu"])
    spread(GRAD_SCALE * jnp.exp(bufs["x_stu"][me, 0:4, :] - stu_peak) / stu_total, part_a)

    def grads(rows, begins):
        stu_scale, tea_scale = part_a[rows, :], part_b[rows, :]
        for i in begins:
            cols = slice(i, i + LANES)
            grad[rows, cols] = (stu_exp[rows, cols] * stu_scale - tea_exp[rows, cols] * tea_scale).astype(BF16)

    ops = []

    def op(name, emit, time, rank, recv=(), send=(), after=()):
        ops.append(
            dict(name=name, emit=emit, time=time, rank=rank, recv=list(recv), send=list(send), after=list(after))
        )

    links = {("y", 0): "y+", ("y", 1): "y-", ("z", 0): "z+", ("z", 1): "z-", ("x", 0): "x+", ("x", 1): "x-"}

    def toward(axis, d):
        return {axis: near(axis, 1 if d == 0 else -1)}

    def signed(d, n):
        return n if d == 0 else -n

    grad_m = bufs["grad_m"]
    high = (y * (3 - y), y - rem2)

    op("g0o", lambda: fourth_m(0), 0.01, -5, recv=[("m", 0, "O")], send=[("c", 262144, ("m", 0, "SO"))])
    op("g0t", lambda: fifth_m(0), 0.78, -5, recv=[("m", 0, "SO")])
    op(
        "g1a",
        lambda: second_m(1),
        0.01,
        -3,
        recv=[("m", 1, "LR0")],
        send=[("x+", 131072, ("m", 1, "O0")), ("x-", 131072, ("m", 1, "O1")), ("c", 262144, ("m", 1, "S0"))],
    )
    op("g1b", lambda: third_m(1), 0.01, -3, recv=[("m", 1, "LR1")], send=[("c", 262144, ("m", 1, "S1"))], after=["g1a"])
    op(
        "g1o",
        lambda: fourth_m(1),
        0.01,
        -3,
        recv=[("m", 1, "O0"), ("m", 1, "O1")],
        send=[("c", 262144, ("m", 1, "SO"))],
        after=["g1b"],
    )
    op("g1t", lambda: fifth_m(1), 0.78, -5, recv=[("m", 1, k) for k in ("SO", "S0", "S1")])

    def chunk(i):
        info = TABLE[i]
        kind, m, w, paired, at, half_at = (info[k] for k in ("kind", "m", "w", "paired", "at", "half"))
        rank = info["rank"]
        pair_link, cross_link = ("p", "q") if m == 0 else ("q", "p")
        partner, cross = partners[m], partners[1 - m]
        opposite = lax.rem(y + 2, NY)
        mine = pl.ds(pl.multiple_of(at + high[m] * (w // 2), LANES), w) if paired else pl.ds(at, w)
        theirs = pl.ds(pl.multiple_of(at + (2 - high[m]) * (w // 2), LANES), w) if paired else None
        got_cols = pl.ds(half_at, w)
        n = 2 if kind == "A" else 4
        z1_s, z1_r, z_s, z_r = (bufs[f"{k}{i}"] for k in ("z1_s", "z1_r", "z_s", "z_r"))
        f_s, f_r = (bufs[f"{k}{i}"] for k in ("f_s", "f_r"))

        def formed(rows_of):
            value = jnp.dot(rows_of(0), grad[:, mine], preferred_element_type=F32)
            if paired:
                value = value + jnp.dot(rows_of(1 + m), grad_m[:, got_cols], preferred_element_type=F32)
            return value

        def cost(rows):
            if kind == "A":
                return 0.71 if w == 128 else 1.1
            return ((0.3 if paired else 0.24) if rows == 256 else (0.22 if paired else 0.19)) * (1 if w == 128 else 1.5)

        start = []
        if paired:

            def emit_swap():
                send(("p", i), grad.at[:, theirs], grad_m.at[:, got_cols], partner)

            def emit_swapped():
                arrive(("p", i), grad_m.at[:, got_cols])

            op(("p", i), emit_swap, 0.02, -10 + 0.01 * info["turn"], send=[(pair_link, 1024 * w, ("p", i))])
            op(("pr", i), emit_swapped, 0.01, rank, recv=[("p", i)], after=[f"g{m}t"])
            start = [("pr", i)]

        if kind == "A":
            a_sum, x_s, x_r = (bufs[f"{k}{i}"] for k in ("a_sum", "x_s", "x_r"))

            def emit_cross():
                for u, j in enumerate((cross["y"], opposite)):
                    x_s[u] = formed(lambda t: hid_t[t, j].reshape(ROWS, ROWS)).astype(BF16)
                send(("q", i), x_s, x_r, cross)

            def emit_kept():
                arrive(("q", i), x_r)
                for u, j in enumerate((y, partner["y"])):
                    value = formed(lambda t: hid_t[t, j].reshape(ROWS, ROWS)) + x_r[u].astype(F32)
                    a_sum[u] = value.reshape(NZ, 64, w)
                f_s[0] = a_sum[1, z].astype(BF16)
                send(("f", i, 0), f_s.at[0], f_r.at[0], partner)

            op(("q", i), emit_cross, cost(1024), rank, send=[(cross_link, 2048 * w, ("q", i))], after=start)
            op(
                ("qf", i),
                emit_kept,
                cost(1024),
                rank,
                recv=[("q", i)],
                send=[(pair_link, 128 * w, ("f", i, 0))],
                after=start,
            )
            start = [("qf", i)]

        def z_part(k, lo, count):
            if kind == "A":
                return a_sum[lo : lo + count, near("z", k)]
            value = formed(lambda t: hid_t[t, lo : lo + count, near("z", k)].reshape(64 * count, ROWS))
            return value.reshape(count, 64, w)

        h = n // 2

        def z_step(d, step):
            dest = signed(d, 5 - step)
            lo = d * h
            src, dst = (z1_s.at[d], z1_r.at[d]) if step == 1 else (z_s.at[d, step - 2], z_r.at[d, step - 2])

            def emit():
                if step == 1:
                    z1_s[d] = z_part(dest, lo, h).astype(BF16)
                elif step == 2:
                    arrive(("z", i, d, 1), z1_r.at[d])
                    z_s[d, 0, h - lo : n - lo] = z_part(dest, h - lo, h).astype(BF16)
                    z_s[d, 0, lo : lo + h] = (z_part(dest, lo, h) + z1_r[d].astype(F32)).astype(BF16)
                else:
                    arrive(("z", i, d, step - 1), z_r.at[d, step - 3])
                    z_s[d, step - 2] = (z_part(dest, 0, n) + z_r[d, step - 3].astype(F32)).astype(BF16)
                if kind == "A" and step == 4:
                    send(("z", i, d, 4), src.at[0], dst.at[0], toward("z", d))
                    send(("f", i, 1 + d), src.at[1], f_r.at[1 + d], {**partner, **toward("z", d)})
                else:
                    send(("z", i, d, step), src, dst, toward("z", d))

            time = 0.012 if kind == "A" else cost(128 if step == 1 else 256)
            alone = kind == "A" and step == 4
            op(
                ("z", i, d, step),
                emit,
                time,
                rank + (FIRST if step == 1 else 0),
                recv=[("z", i, d, step - 1)] if step > 1 else [],
                send=[(links["z", d], 128 * w * (1 if alone else h if step == 1 else n), ("z", i, d, step))]
                + ([(links["z", d], 128 * w, ("f", i, 1 + d))] if alone else []),
                after=start,
            )

        def emit_z_last():
            if kind == "A":
                for d in range(2):
                    arrive(("z", i, d, 4), z_r.at[d, 2, 0])
                gh_out[:, mine] = a_sum[0, z] + z_r[0, 2, 0].astype(F32) + z_r[1, 2, 0].astype(F32)
                return
            z_sum = bufs[f"z_sum{i}"]
            for d in range(2):
                arrive(("z", i, d, 4), z_r.at[d, 2])
            z_sum[...] = z_part(0, 0, n) + z_r[0, 2].astype(F32) + z_r[1, 2].astype(F32)
            for u, device in enumerate((partner, cross, {"y": opposite})):
                f_s[u] = z_sum[device["y"]].astype(BF16)
                send(("f", i, u), f_s.at[u], f_r.at[u], device)

        def emit_last():
            for u in range(3):
                arrive(("f", i, u), f_r.at[u])
            got = [f_r[u].astype(F32) for u in range(3)]
            if kind == "A":
                gh_out[:, theirs] = got[0] + got[1] + got[2]
            elif paired:
                gh_out[:, mine] = bufs[f"z_sum{i}"][y] + got[1]
                gh_out[:, theirs] = got[0] + got[2]
            else:
                gh_out[:, mine] = bufs[f"z_sum{i}"][y] + got[0] + got[1] + got[2]

        for d in range(2):
            for step in range(1, 5):
                z_step(d, step)
        final = [] if kind == "A" else [
            (pair_link, 128 * w, ("f", i, 0)),
            (cross_link, 128 * w, ("f", i, 1)),
            (cross_link, 256 * w, ("f", i, 2)),
        ]
        op(
            ("zf", i),
            emit_z_last,
            0.012 if kind == "A" else cost(256),
            rank,
            recv=[("z", i, d, 4) for d in range(2)],
            send=final,
            after=start,
        )
        op(("ff", i), emit_last, 0.02, rank, recv=[("f", i, u) for u in range(3)], after=[("zf", i)])

    for i in range(len(TABLE)):
        chunk(i)

    hops = (2, 1, 3, 0)

    def back(slot, h):
        return lax.dot_general(
            grad[halves[h], :], head[slot], (((1,), (1,)), ((), ())), preferred_element_type=F32
        )

    def hs_step(n):
        def emit():
            slot = vocab_at(hops[n], 1)
            for h in range(2):
                bufs["hs_s"][n, halves[h], :] = back(slot, h).astype(BF16)
            send(("hs", n), bufs["hs_s"].at[n], bufs["hs_r"].at[n], to_sib)

        op(("hs", n), emit, 0.76, 30, send=[("c", 262144, ("hs", n))])

    def hg_step(n):
        def emit():
            arrive(("hs", n), bufs["hs_r"].at[n])
            if n == 1 or n == 2:
                d = n - 1
                arrive(("h1", d), bufs["h1_r"].at[d])
            if n == 3:
                for d in range(2):
                    arrive(("h2", d), bufs["h2_r"].at[d])
            slot = vocab_at(hops[n], 0)
            for h in range(2):
                rows = halves[h]
                value = back(slot, h) + bufs["hs_r"][n, rows, :].astype(F32)
                if n == 0:
                    bufs["h1_s"][h] = value.astype(BF16)
                    send(("h1", h), bufs["h1_s"].at[h], bufs["h1_r"].at[h], toward("x", h))
                elif n < 3:
                    if h == n - 1:
                        value = value + bufs["h1_r"][h].astype(F32)
                    bufs["h2_s"][n - 1, rows, :] = value.astype(BF16)
                else:
                    got = [bufs["h2_r"][d, rows, :].astype(F32) for d in range(2)]
                    hg_out[rows, :] = (value + got[0] + got[1]).astype(BF16)
            if n == 1 or n == 2:
                d = n - 1
                send(("h2", d), bufs["h2_s"].at[d], bufs["h2_r"].at[d], toward("x", d))

        recv = [("hs", n)] + {0: [], 1: [("h1", 0)], 2: [("h1", 1)], 3: [("h2", 0), ("h2", 1)]}[n]
        sends = {
            0: [("x+", 131072, ("h1", 0)), ("x-", 131072, ("h1", 1))],
            1: [("x+", 262144, ("h2", 0))],
            2: [("x-", 262144, ("h2", 1))],
            3: [],
        }[n]
        op(("hg", n), emit, 0.77 if n else 1.45, 30, recv=recv, send=sends)

    for n in range(4):
        hs_step(n)
        hg_step(n)

    def divergence():
        def emit():
            shared("x_cross")
            ref, peaks = bufs["x_cross"], bufs["x_tea"]
            peak, total = merged(peaks)
            s_peak, s_total = merged(bufs["x_stu"])
            cross = None
            for k in range(8):
                term = ref[k, 0:4, :] * jnp.exp(peaks[k, 0:4, :] - peak)
                cross = term if cross is None else cross + term
            kl_out[...] = cross / total - peak - jnp.log(total) + s_peak + jnp.log(s_total)

        op("kl", emit, 0.05, 40, after=[("hg", 3)])

    divergence()

    order, _ = in_order(ops)
    swaps = [step for step in order if step["name"][0] == "p"]
    early = [step for step in swaps if step["name"][1] in SWAP_FIRST]
    ranges = [(TABLE[i]["at"], TABLE[i]["at"] + 2 * TABLE[i]["w"]) for i in SWAP_FIRST]
    tiles = [[b for b in range(0, VOCAB, LANES) if any(lo <= b < hi for lo, hi in ranges) == first] for first in (True, False)]
    row_blocks(16, lambda rows: grads(rows, tiles[0]))
    for step in early:
        step["emit"]()
    row_blocks(16, lambda rows: grads(rows, tiles[1]))
    for step in order:
        if step not in early:
            step["emit"]()

    for copy in sent:
        copy.wait_send()


def per_device(hidden_states, teacher_logits, head_weight):
    vmem = pl.BlockSpec(memory_space=pltpu.VMEM)
    hbm = pl.BlockSpec(memory_space=pl.ANY)
    kl, hidden_grad, head_grad = pl.pallas_call(
        kernel,
        out_shape=(
            pltpu.VMEM((4, LANES), F32),
            pltpu.VMEM((ROWS, PART), BF16),
            pltpu.VMEM((64, VOCAB), F32),
        ),
        in_specs=[hbm, hbm, hbm],
        out_specs=(vmem, vmem, vmem),
        scratch_shapes=[pltpu.VMEM(*SCRATCH[k]) for k in NAMES]
        + [
            pltpu.SemaphoreType.DMA((10,)),
            pltpu.SemaphoreType.DMA((N_COPIES,)),
            pltpu.SemaphoreType.DMA((N_COPIES,)),
        ],
        compiler_params=pltpu.CompilerParams(
            collective_id=0, has_side_effects=True, vmem_limit_bytes=64_500_000
        ),
    )(hidden_states, teacher_logits, head_weight)
    return kl.reshape(ROWS), hidden_grad, head_grad


def solution(mesh):
    split = Mesh(mesh.devices.reshape(NY, NZ, NX, 2), ("y", "z", "x", "c"))
    dp, vocab = ("y", "z"), ("x", "c")
    return jax.shard_map(
        per_device,
        mesh=split,
        in_specs=(P(dp, vocab), P(dp, vocab), P(None, vocab)),
        out_specs=(P(dp), P(dp, vocab), P(dp, vocab)),
        check_vma=False,
    )
```
